256 devices in a mesh: seq: 32 (over y, z), batch: 8 (over x, core).
Axes of the slice: x: 4, y: 4, z: 8, core: 2. Of those that a mesh axis runs over, the one named last changes fastest.
Arguments:
- conv_input: bfloat16 [32768, 8192], P(('batch', 'seq')), parts along dimension 0, may hold values from -6 to 6
- gate_input: bfloat16 [32768, 8192], P(('batch', 'seq')), parts along dimension 0, may hold values from -6 to 6
- conv_weight: bfloat16 [4, 8192], P(None, 'seq'), may hold values from -3 to 3
- conv_bias: bfloat16 [8192], P('seq'), may hold values from -3 to 3
- x_weight: bfloat16 [8192, 288], P('seq'), may hold values from -0.0625 to 0.0625
- dt_gain: float32 [256], replicated, may hold values from 0.5 to 1.5
- dt_weight: bfloat16 [256, 8192], P(None, 'seq'), may hold values from -0.375 to 0.375
- dt_bias: float32 [8192], P('seq'), may hold values from -6.9 to -2.3
- a_log: float32 [16, 8192], P(None, 'seq'), may hold values from 0 to 2.77
- skip: float32 [8192], P('seq'), may hold values from 0.5 to 1.5
Outputs:
- mixed: bfloat16 [32768, 8192], P(('batch', 'seq')), parts along dimension 0
The draws below stay inside these ranges and needn't reach their ends.
There are 8 independent parts, one for each index of `batch`. The reference program is written for one: setup_inputs(seed, part) draws one part's arguments, and reference() takes and returns one part's arrays. A program takes and returns all parts, laid end to end along the dimension named above; an argument that names none is the same for every part. Nothing has to cross between parts.
All inputs are finite; a program needn't handle non-finite values.
Results may differ from the reference program's by a relative error of at most 0.0085.
Values may be sent and summed in bfloat16 or wider, within the bound.
No kernel may reach another device: no remote copies, remote signals or barrier semaphores. Data moves between devices by JAX's collectives and lax.ppermute only.
A program may use at most 128 MiB of HBM per device.

```python
import jax
import jax.numpy as jnp
from jax import lax

INNER = 8192
STATE = 16
DT_RANK = 256
CONV = 4
LENGTH = 4096
PROJ = 288


def block_scale(key, extent, pieces, low, top_value):
    def one(axis_at, blocks):
        steps = jax.random.uniform(jax.random.fold_in(jax.random.fold_in(key, 6), axis_at), (blocks,), jnp.float32, low / len(pieces), top_value / len(pieces))
        return jnp.repeat(jnp.exp(steps), extent[axis_at] // blocks).reshape((-1,) + (1,) * (len(extent) - axis_at - 1))

    loudness = one(*pieces[0])
    for cut in pieces[1:]:
        loudness = loudness * one(*cut)
    return loudness


def centred(stream_key, shape, scale, limit, shards=(), kind=jnp.bfloat16):
    drawn = scale * jax.random.normal(stream_key, shape, jnp.float32)
    if shards:
        drawn = drawn * block_scale(stream_key, shape, shards, -0.22, 0.18)
    return jnp.clip(drawn, -limit, limit).astype(kind)


def setup_inputs(seed: int = 0, part: int = 0) -> dict:
    key_list = jax.random.split(jax.random.key(seed), 11)
    part_splits = jax.random.split(jax.random.fold_in(key_list[10], part), 11)
    conv_input = centred(part_splits[0], (LENGTH, INNER), 1.0, 6.0, ((0, 32),))
    gate_input = centred(part_splits[1], (LENGTH, INNER), 1.0, 6.0, ((0, 32),))
    conv_weight = centred(key_list[2], (CONV, INNER), CONV ** -0.5, 3.0, ((1, 32),))
    conv_bias = centred(key_list[3], (INNER,), 0.5, 3.0, ((0, 32),))
    x_weight = centred(key_list[4], (INNER, PROJ), INNER ** -0.5, 0.0625, ((0, 32),))
    dt_gain = jnp.clip(1.0 + 0.1 * jax.random.normal(key_list[5], (DT_RANK,), jnp.float32), 0.5, 1.5)
    dt_weight = centred(key_list[6], (DT_RANK, INNER), DT_RANK ** -0.5, 0.375, ((1, 32),))
    dt_bias = jnp.clip(-6.9 + 4.6000001430511475 * jax.random.uniform(key_list[7], (INNER,), jnp.float32) ** block_scale(key_list[7], (INNER,), ((0, 32),), -0.2, 0.2), -6.9, -2.3)
    a_log = jnp.clip(2.77 * jax.random.uniform(key_list[8], (STATE, INNER), jnp.float32) ** block_scale(key_list[8], (STATE, INNER), ((1, 32),), -0.2, 0.2), 0.0, 2.77)
    skip = jnp.clip(1.0 + 0.1 * jax.random.normal(key_list[9], (INNER,), jnp.float32), 0.5, 1.5)
    return dict(conv_input=conv_input, gate_input=gate_input, conv_weight=conv_weight, conv_bias=conv_bias, x_weight=x_weight, dt_gain=dt_gain, dt_weight=dt_weight, dt_bias=dt_bias, a_log=a_log, skip=skip)


def convolve(inputs, weight, bias):
    rows = inputs.shape[0]
    width = weight.shape[0]
    padded = jnp.concatenate([jnp.zeros((width - 1, inputs.shape[1]), jnp.float32), inputs.astype(jnp.float32)], 0)
    total = bias.astype(jnp.float32)[None, :]
    for tap in range(width):
        total = total + weight[tap].astype(jnp.float32)[None, :] * padded[tap:tap + rows]
    return jax.nn.silu(total).astype(jnp.bfloat16)

def reference(conv_input, gate_input, conv_weight, conv_bias, x_weight, dt_gain, dt_weight, dt_bias, a_log, skip):
    xc = convolve(conv_input, conv_weight, conv_bias)
    proj = jnp.dot(xc, x_weight, preferred_element_type=jnp.float32)
    dt_low = proj[:, :DT_RANK]
    bmat = proj[:, DT_RANK:DT_RANK + STATE]
    cmat = proj[:, DT_RANK + STATE:]
    normed = (dt_low * lax.rsqrt(lax.optimization_barrier(jnp.mean(dt_low * dt_low, axis=1, keepdims=True)) + 1e-06) * dt_gain[None, :]).astype(jnp.bfloat16)
    step = jax.nn.softplus(jnp.dot(normed, dt_weight, preferred_element_type=jnp.float32) + dt_bias[None, :])
    rate = -jnp.exp(a_log)
    xfloat = xc.astype(jnp.float32)

    def advance(state, inputs):
        step_t, x_t, b_t, c_t = inputs
        state = jnp.exp(step_t[None, :] * rate) * state + b_t[:, None] * (step_t * x_t)[None, :]
        return (state, lax.optimization_barrier(jnp.sum(c_t[:, None] * state, axis=0)))
    _, outputs = lax.scan(advance, jnp.zeros((STATE, INNER), jnp.float32), (step, xfloat, bmat, cmat))
    y_out = (outputs + skip[None, :] * xfloat).astype(jnp.bfloat16)
    y_out = lax.optimization_barrier(y_out)
    return (y_out.astype(jnp.float32) * jax.nn.silu(gate_input.astype(jnp.float32))).astype(jnp.bfloat16)
```

```python
import jax
import jax.numpy as jnp
from jax import lax
from jax.experimental import pallas as pl
from jax.experimental.pallas import tpu as pltpu
from jax.sharding import Mesh, PartitionSpec as P

F32 = jnp.float32
BF16 = jnp.bfloat16
LOG2E = 1.4426950408889634
SEQ = ("y", "z")
BLK = 1024
SHARD = 256


def silu(v):
    return v / (1.0 + jnp.exp(-v))


def row_of(ref, at):
    return ref[pl.ds(at, 8, stride=0), :]


def two_parts(v):
    high = lax.reduce_precision(v, 8, 7)
    return high.astype(BF16), (v - high).astype(BF16)


def front_kernel(core_ref, ci_ref, prior_ref, own_ref, oth_ref, gain_ref, xc_ref, normed_ref, bc_ref, pad_ref, acc_ref):
    step = pl.program_id(0)
    core = core_ref[0]
    rows = ci_ref.shape[0]
    taps = 4
    pad_ref[0:8, :] = prior_ref[...].astype(F32)
    pad_ref[8 : 8 + rows, :] = ci_ref[...].astype(F32)

    @pl.when(step == 0)
    def _():
        acc_ref[...] = jnp.zeros_like(acc_ref)

    acc = acc_ref[...]
    for s in range(4):
        mine = own_ref[s, 0, 128:136, 0:SHARD].astype(F32)
        other = oth_ref[s, 0, 128:136, 0:SHARD].astype(F32)
        par = jnp.where(core == 0, mine, other)
        lanes = slice(s * SHARD, (s + 1) * SHARD)
        total = jnp.broadcast_to(par[taps : taps + 1, :], (rows, SHARD))
        for k in range(taps):
            total = total + par[k : k + 1, :] * pad_ref[5 + k : 5 + k + rows, lanes]
        xc_ref[:, lanes] = silu(total).astype(BF16)
        at = pl.multiple_of(s * SHARD + core * 128, 128)
        acc = acc + jnp.dot(xc_ref[:, pl.ds(at, 128)], own_ref[s, 0, 0:128, :], preferred_element_type=F32)
        at = pl.multiple_of(s * SHARD + (1 - core) * 128, 128)
        acc = acc + jnp.dot(xc_ref[:, pl.ds(at, 128)], oth_ref[s, 0, 0:128, :], preferred_element_type=F32)
    acc_ref[...] = acc

    @pl.when(step == pl.num_programs(0) - 1)
    def _():
        rank = gain_ref.shape[1]
        low = acc_ref[:, 0:rank]
        scale = lax.rsqrt(jnp.mean(low * low, axis=1, keepdims=True) + 1e-06)
        normed_ref[...] = (low * scale * gain_ref[...]).astype(BF16)
        for m in range(32):
            col = acc_ref[:, rank + m : rank + m + 1]
            bc_ref[m * rows : (m + 1) * rows, :] = jnp.broadcast_to(col, (rows, 128))


def front(core, conv_input, prior, x_own, x_oth, gain):
    rows, inner = conv_input.shape
    wspec = pl.BlockSpec((4, 1, 136, 288), lambda b: (b % 2, b // 2, 0, 0))
    return pl.pallas_call(
        front_kernel,
        grid=(inner // BLK,),
        in_specs=[
            pl.BlockSpec(memory_space=pltpu.SMEM),
            pl.BlockSpec((rows, BLK), lambda b: (0, b)),
            pl.BlockSpec((8, BLK), lambda b: (0, b)),
            wspec,
            wspec,
            pl.BlockSpec((1, 256), lambda b: (0, 0)),
        ],
        out_specs=[
            pl.BlockSpec((rows, BLK), lambda b: (0, b)),
            pl.BlockSpec((rows, 256), lambda b: (0, 0)),
            pl.BlockSpec((32 * rows, 128), lambda b: (0, 0)),
        ],
        out_shape=[
            jax.ShapeDtypeStruct((rows, inner), BF16),
            jax.ShapeDtypeStruct((rows, 256), BF16),
            jax.ShapeDtypeStruct((32 * rows, 128), F32),
        ],
        scratch_shapes=[pltpu.VMEM((rows + 8, BLK), F32), pltpu.VMEM((rows, 288), F32)],
        compiler_params=pltpu.CompilerParams(dimension_semantics=("arbitrary",)),
        name="front",
    )(core, conv_input, prior, x_own, x_oth, gain)


def scan_kernel(core_ref, normed_ref, xc_ref, own_ref, oth_ref, bc_ref, step_ref, y_ref, rate_ref, ends_ref, x_scr, par_scr, h_scr):
    core = core_ref[0]
    rows = normed_ref.shape[0]
    mine_k = normed_ref[:, pl.ds(pl.multiple_of(core * 128, 128), 128)]
    other_k = normed_ref[:, pl.ds(pl.multiple_of((1 - core) * 128, 128), 128)]
    skips = []
    for s in range(4):
        raw = jnp.dot(mine_k, own_ref[s, 0, 0:128, :], preferred_element_type=F32)
        raw = raw + jnp.dot(other_k, oth_ref[s, 0, 0:128, :], preferred_element_type=F32)
        mine = own_ref[s, 0, 128:152, :].astype(F32)
        other = oth_ref[s, 0, 128:152, :].astype(F32)
        mine_log = mine[0:8] + mine[8:16]
        other_log = other[0:8] + other[8:16]
        mine_vec = mine[16:17] + mine[17:18]
        other_vec = other[16:17] + other[17:18]
        bias = jnp.where(core == 0, mine_vec, other_vec)
        skip = jnp.where(core == 0, other_vec, mine_vec)
        raw = raw + bias
        step = jnp.maximum(raw, 0.0) + jnp.log1p(jnp.exp(-jnp.abs(raw)))
        xs = xc_ref[:, s * SHARD : (s + 1) * SHARD].astype(F32)
        for p in range(2):
            j = 2 * s + p
            lanes = slice(p * 128, (p + 1) * 128)
            for i in range(rows // 8):
                step_ref[0, pl.ds(64 * i + j, 8, stride=8), :] = step[8 * i : 8 * i + 8, lanes]
                x_scr[pl.ds(64 * i + j, 8, stride=8), :] = xs[8 * i : 8 * i + 8, lanes]
            at = pl.multiple_of(j * 16 + core * 8, 8)
            par_scr[pl.ds(at, 8), :] = -LOG2E * jnp.exp(mine_log[:, lanes])
            at = pl.multiple_of(j * 16 + (1 - core) * 8, 8)
            par_scr[pl.ds(at, 8), :] = -LOG2E * jnp.exp(other_log[:, lanes])
            skips.append(skip[:, lanes])
    skip = jnp.concatenate(skips, 0)
    for n in range(16):
        rate_ref[0, 8 * n : 8 * n + 8, :] = par_scr[pl.ds(n, 8, stride=16), :]
    rates = [rate_ref[0, 8 * n : 8 * n + 8, :] for n in range(16)]

    def advance(t, carry):
        total, state = carry
        at = pl.multiple_of(t * 8, 8)
        now = step_ref[0, pl.ds(at, 8), :]
        xt = x_scr[pl.ds(at, 8), :]
        drive = now * xt
        even = skip * xt
        odd = None
        fresh = []
        for n in range(16):
            b = row_of(bc_ref, n * rows + t)
            c = row_of(bc_ref, (16 + n) * rows + t)
            h = jnp.exp2(now * rates[n]) * state[n] + b * drive
            fresh.append(h)
            if n % 2:
                odd = c * h if odd is None else odd + c * h
            else:
                even = even + c * h
        y_ref[0, pl.ds(at, 8), :] = even + odd
        return total + now, tuple(fresh)

    zero = jnp.zeros((8, 128), F32)
    total, state = lax.fori_loop(0, rows, advance, (zero, (zero,) * 16))
    for n in range(16):
        h_scr[8 * n : 8 * n + 8, :] = state[n]
    high = total.astype(BF16).astype(F32)
    h_scr[128:136, :] = high
    h_scr[136:144, :] = total - high
    for j in range(8):
        low = h_scr[pl.ds(j, 8, stride=8), :]
        up = h_scr[pl.ds(64 + j, 8, stride=8), :]
        ends_ref[j // 2, (j % 2) * 16 : (j % 2) * 16 + 16, :] = jnp.concatenate([low, up], 0).astype(BF16)
    for jj in range(4):
        sums = [h_scr[128 + 2 * jj : 130 + 2 * jj, :], h_scr[136 + 2 * jj : 138 + 2 * jj, :], jnp.zeros((4, 128), F32)]
        ends_ref[jj, 32:40, :] = jnp.concatenate(sums, 0).astype(BF16)


def scan(core, normed, xc, d_own, d_oth, bc):
    rows, inner = xc.shape
    blocks = inner // BLK
    wspec = pl.BlockSpec((4, 1, 152, 256), lambda b: (b % 2, b // 2, 0, 0))
    return pl.pallas_call(
        scan_kernel,
        grid=(blocks,),
        in_specs=[
            pl.BlockSpec(memory_space=pltpu.SMEM),
            pl.BlockSpec((rows, 256), lambda b: (0, 0)),
            pl.BlockSpec((rows, BLK), lambda b: (0, b)),
            wspec,
            wspec,
            pl.BlockSpec((32 * rows, 128), lambda b: (0, 0)),
        ],
        out_specs=[
            pl.BlockSpec((1, 8 * rows, 128), lambda b: (b, 0, 0)),
            pl.BlockSpec((1, 8 * rows, 128), lambda b: (b, 0, 0)),
            pl.BlockSpec((1, 128, 128), lambda b: (b, 0, 0)),
            pl.BlockSpec((4, 40, 128), lambda b: (b, 0, 0)),
        ],
        out_shape=[
            jax.ShapeDtypeStruct((blocks, 8 * rows, 128), F32),
            jax.ShapeDtypeStruct((blocks, 8 * rows, 128), F32),
            jax.ShapeDtypeStruct((blocks, 128, 128), F32),
            jax.ShapeDtypeStruct((4 * blocks, 40, 128), BF16),
        ],
        scratch_shapes=[
            pltpu.VMEM((8 * rows, 128), F32),
            pltpu.VMEM((128, 128), F32),
            pltpu.VMEM((144, 128), F32),
        ],
        compiler_params=pltpu.CompilerParams(dimension_semantics=("arbitrary",)),
        name="scan",
    )(core, normed, xc, d_own, d_oth, bc)


def link_kernel(ends_ref, log_ref, start_ref):
    count = ends_ref.shape[0]
    rate = -LOG2E * jnp.exp(log_ref[...])
    rate = jnp.concatenate([rate[:, 0:128], rate[:, 128:256]], 0)
    state = jnp.zeros((32, 128), F32)
    for s in range(count):
        start_ref[s] = state.astype(BF16)
        sums = ends_ref[s, 32:40, :].astype(F32)
        sums = sums[0:2] + sums[2:4]
        spread = jnp.concatenate([jnp.broadcast_to(sums[0:1], (16, 128)), jnp.broadcast_to(sums[1:2], (16, 128))], 0)
        state = jnp.exp2(rate * spread) * state + ends_ref[s, 0:32, :].astype(F32)


def link(ends, a_log):
    return pl.pallas_call(
        link_kernel,
        out_shape=jax.ShapeDtypeStruct((ends.shape[0], 32, 128), BF16),
        name="link",
    )(ends, a_log)


def close_kernel(step_ref, y_ref, rate_ref, start_ref, c_ref, gate_ref, out_ref, s_scr, y_scr):
    rows = gate_ref.shape[0]
    for j in range(8):
        s_scr[16 * j : 16 * j + 16, :] = start_ref[j // 2, (j % 2) * 16 : (j % 2) * 16 + 16, :].astype(F32)
    starts = [s_scr[pl.ds(n, 8, stride=16), :] for n in range(16)]
    rates = [rate_ref[0, 8 * n : 8 * n + 8, :] for n in range(16)]

    def advance(t, total):
        at = pl.multiple_of(t * 8, 8)
        total = total + step_ref[0, pl.ds(at, 8), :]
        even = y_ref[0, pl.ds(at, 8), :]
        odd = None
        for n in range(16):
            c = row_of(c_ref, n * rows + t)
            part = c * starts[n] * jnp.exp2(total * rates[n])
            if n % 2:
                odd = part if odd is None else odd + part
            else:
                even = even + part
        y_scr[pl.ds(at, 8), :] = even + odd
        return total

    lax.fori_loop(0, rows, advance, jnp.zeros((8, 128), F32))
    for j in range(8):
        for i in range(rows // 16):
            low = y_scr[pl.ds(128 * i + j, 8, stride=8), :]
            up = y_scr[pl.ds(128 * i + 64 + j, 8, stride=8), :]
            y = jnp.concatenate([low, up], 0).astype(BF16).astype(F32)
            gate = gate_ref[16 * i : 16 * i + 16, j * 128 : (j + 1) * 128].astype(F32)
            out_ref[16 * i : 16 * i + 16, j * 128 : (j + 1) * 128] = (y * silu(gate)).astype(BF16)


def close(step, y, rate, start, bc, gate):
    rows, inner = gate.shape
    return pl.pallas_call(
        close_kernel,
        grid=(inner // BLK,),
        in_specs=[
            pl.BlockSpec((1, 8 * rows, 128), lambda b: (b, 0, 0)),
            pl.BlockSpec((1, 8 * rows, 128), lambda b: (b, 0, 0)),
            pl.BlockSpec((1, 128, 128), lambda b: (b, 0, 0)),
            pl.BlockSpec((4, 32, 128), lambda b: (b, 0, 0)),
            pl.BlockSpec((16 * rows, 128), lambda b: (1, 0)),
            pl.BlockSpec((rows, BLK), lambda b: (0, b)),
        ],
        out_specs=pl.BlockSpec((rows, BLK), lambda b: (0, b)),
        out_shape=jax.ShapeDtypeStruct((rows, inner), BF16),
        scratch_shapes=[pltpu.VMEM((128, 128), F32), pltpu.VMEM((8 * rows, 128), F32)],
        compiler_params=pltpu.CompilerParams(dimension_semantics=("arbitrary",)),
        name="close",
    )(step, y, rate, start, bc, gate)


def from_everyone(x, axis):
    copies = jnp.broadcast_to(x, (lax.axis_size(axis), *x.shape))
    return lax.all_to_all(copies, axis, split_axis=0, concat_axis=0, tiled=True)


def pack_x(core, x_weight, conv_weight, conv_bias):
    half = lax.dynamic_slice_in_dim(x_weight, core * 128, 128, 0)
    extra = jnp.concatenate([conv_weight, conv_bias[None, :], jnp.zeros((3, SHARD), BF16)], 0)
    return jnp.concatenate([half, jnp.pad(extra, ((0, 0), (0, 32)))], 0)


def pack_d(core, dt_weight, dt_bias, a_log, skip):
    half = lax.dynamic_slice_in_dim(dt_weight, core * 128, 128, 0)
    logs = lax.dynamic_slice_in_dim(a_log, core * 8, 8, 0)
    vec = jnp.where(core == 0, dt_bias, skip)[None, :]
    pieces = [half, *two_parts(logs), *two_parts(vec), jnp.zeros((6, SHARD), BF16)]
    return jnp.concatenate(pieces, 0)


def local(conv_input, gate_input, conv_weight, conv_bias, x_weight, dt_gain, dt_weight, dt_bias, a_log, skip):
    core = lax.axis_index("core")
    count = lax.axis_size(SEQ)
    swap = [(0, 1), (1, 0)]
    x_part = from_everyone(pack_x(core, x_weight, conv_weight, conv_bias), "y")
    x_own = lax.all_gather(x_part, "z", axis=0)
    d_part = from_everyone(pack_d(core, dt_weight, dt_bias, a_log, skip), "y")
    d_own = lax.all_gather(d_part, "z", axis=0)
    x_oth = lax.ppermute(x_own, "core", swap)
    d_oth = lax.ppermute(d_own, "core", swap)
    prior = lax.ppermute(conv_input[conv_input.shape[0] - 8 :], SEQ, [(i, i + 1) for i in range(count - 1)])
    which = core.reshape(1).astype(jnp.int32)
    xc, normed, bc = front(which, conv_input, prior, x_own, x_oth, dt_gain[None, :])
    step, y, rate, ends = scan(which, normed, xc, d_own, d_oth, bc)
    ends = lax.all_to_all(ends, SEQ, split_axis=0, concat_axis=0, tiled=True)
    ends = ends.reshape(count, 40, 128)
    start = lax.all_to_all(link(ends, a_log), SEQ, split_axis=0, concat_axis=0, tiled=True)
    return close(step, y, rate, start, bc, gate_input)


def solution(mesh):
    inner = Mesh(mesh.devices.reshape(4, 8, 4, 2), ("y", "z", "x", "core"))
    tokens = P(("x", "core", "y", "z"), None)
    return jax.shard_map(
        local,
        mesh=inner,
        in_specs=(tokens, tokens, P(None, SEQ), P(SEQ), P(SEQ, None), P(), P(None, SEQ), P(SEQ), P(None, SEQ), P(SEQ)),
        out_specs=tokens,
        check_vma=False,
    )
```

```python
import jax
import jax.numpy as jnp
from jax import lax
from jax.experimental import pallas as pl
from jax.experimental.pallas import tpu as pltpu
from jax.sharding import Mesh, PartitionSpec as P

F32 = jnp.float32
BF16 = jnp.bfloat16
LOG2E = 1.4426950408889634
SEQ = ("y", "z")
BLK = 1024
SHARD = 256


def silu(v):
    return v / (1.0 + jnp.exp(-v))


def row_of(ref, at):
    return ref[pl.ds(at, 8, stride=0), :]


def two_parts(v):
    high = lax.reduce_precision(v, 8, 7)
    return high.astype(BF16), (v - high).astype(BF16)


def conv_kernel(ci_ref, prior_ref, par_ref, xc_ref, pad_ref):
    rows = ci_ref.shape[0]
    taps = 4
    pad_ref[0:8, :] = prior_ref[...].astype(F32)
    pad_ref[8 : 8 + rows, :] = ci_ref[...].astype(F32)
    for s in range(4):
        par = par_ref[s, 0].astype(F32)
        lanes = slice(s * SHARD, (s + 1) * SHARD)
        total = jnp.broadcast_to(par[taps : taps + 1, :], (rows, SHARD))
        for k in range(taps):
            total = total + par[k : k + 1, :] * pad_ref[5 + k : 5 + k + rows, lanes]
        xc_ref[:, lanes] = silu(total).astype(BF16)


def conv(conv_input, prior, params):
    rows, inner = conv_input.shape
    return pl.pallas_call(
        conv_kernel,
        grid=(inner // BLK,),
        in_specs=[
            pl.BlockSpec((rows, BLK), lambda b: (0, b)),
            pl.BlockSpec((8, BLK), lambda b: (0, b)),
            pl.BlockSpec((4, 1, 8, SHARD), lambda b: (b % 2, b // 2, 0, 0)),
        ],
        out_specs=pl.BlockSpec((rows, BLK), lambda b: (0, b)),
        out_shape=jax.ShapeDtypeStruct((rows, inner), BF16),
        scratch_shapes=[pltpu.VMEM((rows + 8, BLK), F32)],
        compiler_params=pltpu.CompilerParams(dimension_semantics=("arbitrary",)),
        name="conv",
    )(conv_input, prior, params)


def front_kernel(core_ref, xc_ref, own_ref, oth_ref, gain_ref, normed_ref, bc_ref, acc_ref):
    step = pl.program_id(0)
    core = core_ref[0]
    rows = xc_ref.shape[0]

    @pl.when(step == 0)
    def _():
        acc_ref[...] = jnp.zeros_like(acc_ref)

    acc = acc_ref[...]
    for s in range(4):
        at = pl.multiple_of(s * SHARD + core * 128, 128)
        acc = acc + jnp.dot(xc_ref[:, pl.ds(at, 128)], own_ref[s, 0], preferred_element_type=F32)
        at = pl.multiple_of(s * SHARD + (1 - core) * 128, 128)
        acc = acc + jnp.dot(xc_ref[:, pl.ds(at, 128)], oth_ref[s, 0], preferred_element_type=F32)
    acc_ref[...] = acc

    @pl.when(step == pl.num_programs(0) - 1)
    def _():
        rank = gain_ref.shape[1]
        low = acc_ref[:, 0:rank]
        scale = lax.rsqrt(jnp.mean(low * low, axis=1, keepdims=True) + 1e-06)
        normed_ref[...] = (low * scale * gain_ref[...]).astype(BF16)
        for m in range(32):
            col = acc_ref[:, rank + m : rank + m + 1]
            bc_ref[m * rows : (m + 1) * rows, :] = jnp.broadcast_to(col, (rows, 128))


def front(core, xc, x_own, x_oth, gain):
    rows, inner = xc.shape
    wspec = pl.BlockSpec((4, 1, 128, 288), lambda b: (b % 2, b // 2, 0, 0))
    return pl.pallas_call(
        front_kernel,
        grid=(inner // BLK,),
        in_specs=[
            pl.BlockSpec(memory_space=pltpu.SMEM),
            pl.BlockSpec((rows, BLK), lambda b: (0, b)),
            wspec,
            wspec,
            pl.BlockSpec((1, 256), lambda b: (0, 0)),
        ],
        out_specs=[
            pl.BlockSpec((rows, 256), lambda b: (0, 0)),
            pl.BlockSpec((32 * rows, 128), lambda b: (0, 0)),
        ],
        out_shape=[
            jax.ShapeDtypeStruct((rows, 256), BF16),
            jax.ShapeDtypeStruct((32 * rows, 128), F32),
        ],
        scratch_shapes=[pltpu.VMEM((rows, 288), F32)],
        compiler_params=pltpu.CompilerParams(dimension_semantics=("arbitrary",)),
        name="front",
    )(core, xc, x_own, x_oth, gain)


def scan_kernel(where_ref, normed_ref, xc_ref, own_ref, oth_ref, bc_ref, step_ref, y_ref, rate_ref, ends_ref, x_scr, par_scr, h_scr):
    core = where_ref[0]
    rows = normed_ref.shape[0]
    mine_k = normed_ref[:, pl.ds(pl.multiple_of(core * 128, 128), 128)]
    other_k = normed_ref[:, pl.ds(pl.multiple_of((1 - core) * 128, 128), 128)]
    skips = []
    for s in range(4):
        raw = jnp.dot(mine_k, own_ref[0, s, 0:128, :], preferred_element_type=F32)
        raw = raw + jnp.dot(other_k, oth_ref[0, s, 0:128, :], preferred_element_type=F32)
        mine = own_ref[0, s, 128:152, :].astype(F32)
        other = oth_ref[0, s, 128:152, :].astype(F32)
        mine_log = mine[0:8] + mine[8:16]
        other_log = other[0:8] + other[8:16]
        mine_vec = mine[16:17] + mine[17:18]
        other_vec = other[16:17] + other[17:18]
        bias = jnp.where(core == 0, mine_vec, other_vec)
        skip = jnp.where(core == 0, other_vec, mine_vec)
        raw = raw + bias
        step = jnp.maximum(raw, 0.0) + jnp.log1p(jnp.exp(-jnp.abs(raw)))
        xs = xc_ref[:, s * SHARD : (s + 1) * SHARD].astype(F32)
        for p in range(2):
            j = 2 * s + p
            lanes = slice(p * 128, (p + 1) * 128)
            for i in range(rows // 8):
                step_ref[0, pl.ds(64 * i + j, 8, stride=8), :] = step[8 * i : 8 * i + 8, lanes]
                x_scr[pl.ds(64 * i + j, 8, stride=8), :] = xs[8 * i : 8 * i + 8, lanes]
            at = pl.multiple_of(j * 16 + core * 8, 8)
            par_scr[pl.ds(at, 8), :] = -LOG2E * jnp.exp(mine_log[:, lanes])
            at = pl.multiple_of(j * 16 + (1 - core) * 8, 8)
            par_scr[pl.ds(at, 8), :] = -LOG2E * jnp.exp(other_log[:, lanes])
            skips.append(skip[:, lanes])
    skip = jnp.concatenate(skips, 0)
    for n in range(16):
        rate_ref[0, 8 * n : 8 * n + 8, :] = par_scr[pl.ds(n, 8, stride=16), :]
    rates = [rate_ref[0, 8 * n : 8 * n + 8, :] for n in range(16)]

    def advance(t, carry):
        total, state = carry
        at = pl.multiple_of(t * 8, 8)
        now = step_ref[0, pl.ds(at, 8), :]
        xt = x_scr[pl.ds(at, 8), :]
        drive = now * xt
        even = skip * xt
        odd = None
        fresh = []
        for n in range(16):
            b = row_of(bc_ref, n * rows + t)
            c = row_of(bc_ref, (16 + n) * rows + t)
            h = jnp.exp2(now * rates[n]) * state[n] + b * drive
            fresh.append(h)
            if n % 2:
                odd = c * h if odd is None else odd + c * h
            else:
                even = even + c * h
        y_ref[0, pl.ds(at, 8), :] = even + odd
        return total + now, tuple(fresh)

    zero = jnp.zeros((8, 128), F32)
    total, state = lax.fori_loop(0, rows, advance, (zero, (zero,) * 16), unroll=4)
    for n in range(16):
        h_scr[8 * n : 8 * n + 8, :] = state[n]
    high = total.astype(BF16).astype(F32)
    h_scr[128:136, :] = high
    h_scr[136:144, :] = total - high
    for j in range(8):
        low = h_scr[pl.ds(j, 8, stride=8), :]
        up = h_scr[pl.ds(64 + j, 8, stride=8), :]
        ends_ref[j // 2, (j % 2) * 16 : (j % 2) * 16 + 16, :] = jnp.concatenate([low, up], 0).astype(BF16)
    for jj in range(4):
        sums = [h_scr[128 + 2 * jj : 130 + 2 * jj, :], h_scr[136 + 2 * jj : 138 + 2 * jj, :], jnp.zeros((4, 128), F32)]
        ends_ref[jj, 32:40, :] = jnp.concatenate(sums, 0).astype(BF16)


def scan(where, normed, xc, d_own, d_oth, bc):
    rows, inner = xc.shape
    blocks = inner // BLK
    wspec = pl.BlockSpec((1, 4, 152, 256), lambda b, where: ((b // 2 + 4 - where[1]) % 4, b % 2, 0, 0))
    grid_spec = pltpu.PrefetchScalarGridSpec(
        num_scalar_prefetch=1,
        grid=(blocks,),
        in_specs=[
            pl.BlockSpec((rows, 256), lambda b, where: (0, 0)),
            pl.BlockSpec((rows, BLK), lambda b, where: (0, b)),
            wspec,
            wspec,
            pl.BlockSpec((32 * rows, 128), lambda b, where: (0, 0)),
        ],
        out_specs=[
            pl.BlockSpec((1, 8 * rows, 128), lambda b, where: (b, 0, 0)),
            pl.BlockSpec((1, 8 * rows, 128), lambda b, where: (b, 0, 0)),
            pl.BlockSpec((1, 128, 128), lambda b, where: (b, 0, 0)),
            pl.BlockSpec((4, 40, 128), lambda b, where: (b, 0, 0)),
        ],
        scratch_shapes=[
            pltpu.VMEM((8 * rows, 128), F32),
            pltpu.VMEM((128, 128), F32),
            pltpu.VMEM((144, 128), F32),
        ],
    )
    return pl.pallas_call(
        scan_kernel,
        grid_spec=grid_spec,
        out_shape=[
            jax.ShapeDtypeStruct((blocks, 8 * rows, 128), F32),
            jax.ShapeDtypeStruct((blocks, 8 * rows, 128), F32),
            jax.ShapeDtypeStruct((blocks, 128, 128), F32),
            jax.ShapeDtypeStruct((4 * blocks, 40, 128), BF16),
        ],
        compiler_params=pltpu.CompilerParams(dimension_semantics=("arbitrary",)),
        name="scan",
    )(where, normed, xc, d_own, d_oth, bc)


def link_kernel(ends_ref, log_ref, start_ref):
    count = ends_ref.shape[0]
    rate = -LOG2E * jnp.exp(log_ref[...])
    rate = jnp.concatenate([rate[:, 0:128], rate[:, 128:256]], 0)
    state = jnp.zeros((32, 128), F32)
    for s in range(count):
        start_ref[s] = state.astype(BF16)
        sums = ends_ref[s, 32:40, :].astype(F32)
        sums = sums[0:2] + sums[2:4]
        spread = jnp.concatenate([jnp.broadcast_to(sums[0:1], (16, 128)), jnp.broadcast_to(sums[1:2], (16, 128))], 0)
        state = jnp.exp2(rate * spread) * state + ends_ref[s, 0:32, :].astype(F32)


def link(ends, a_log):
    return pl.pallas_call(
        link_kernel,
        out_shape=jax.ShapeDtypeStruct((ends.shape[0], 32, 128), BF16),
        name="link",
    )(ends, a_log)


def close_kernel(step_ref, y_ref, rate_ref, start_ref, c_ref, gate_ref, out_ref, s_scr, y_scr):
    rows = gate_ref.shape[0]
    for j in range(8):
        s_scr[16 * j : 16 * j + 16, :] = start_ref[j // 2, (j % 2) * 16 : (j % 2) * 16 + 16, :].astype(F32)
    starts = [s_scr[pl.ds(n, 8, stride=16), :] for n in range(16)]
    rates = [rate_ref[0, 8 * n : 8 * n + 8, :] for n in range(16)]

    def advance(t, total):
        at = pl.multiple_of(t * 8, 8)
        total = total + step_ref[0, pl.ds(at, 8), :]
        even = y_ref[0, pl.ds(at, 8), :]
        odd = None
        for n in range(16):
            c = row_of(c_ref, n * rows + t)
            part = c * starts[n] * jnp.exp2(total * rates[n])
            if n % 2:
                odd = part if odd is None else odd + part
            else:
                even = even + part
        y_scr[pl.ds(at, 8), :] = even + odd
        return total

    lax.fori_loop(0, rows, advance, jnp.zeros((8, 128), F32), unroll=4)
    for j in range(8):
        for i in range(rows // 16):
            low = y_scr[pl.ds(128 * i + j, 8, stride=8), :]
            up = y_scr[pl.ds(128 * i + 64 + j, 8, stride=8), :]
            y = jnp.concatenate([low, up], 0).astype(BF16).astype(F32)
            gate = gate_ref[16 * i : 16 * i + 16, j * 128 : (j + 1) * 128].astype(F32)
            out_ref[16 * i : 16 * i + 16, j * 128 : (j + 1) * 128] = (y * silu(gate)).astype(BF16)


def close(step, y, rate, start, bc, gate):
    rows, inner = gate.shape
    return pl.pallas_call(
        close_kernel,
        grid=(inner // BLK,),
        in_specs=[
            pl.BlockSpec((1, 8 * rows, 128), lambda b: (b, 0, 0)),
            pl.BlockSpec((1, 8 * rows, 128), lambda b: (b, 0, 0)),
            pl.BlockSpec((1, 128, 128), lambda b: (b, 0, 0)),
            pl.BlockSpec((4, 32, 128), lambda b: (b, 0, 0)),
            pl.BlockSpec((16 * rows, 128), lambda b: (1, 0)),
            pl.BlockSpec((rows, BLK), lambda b: (0, b)),
        ],
        out_specs=pl.BlockSpec((rows, BLK), lambda b: (0, b)),
        out_shape=jax.ShapeDtypeStruct((rows, inner), BF16),
        scratch_shapes=[pltpu.VMEM((128, 128), F32), pltpu.VMEM((8 * rows, 128), F32)],
        compiler_params=pltpu.CompilerParams(dimension_semantics=("arbitrary",)),
        name="close",
    )(step, y, rate, start, bc, gate)


def from_everyone(x, axis):
    copies = jnp.broadcast_to(x, (lax.axis_size(axis), *x.shape))
    return lax.all_to_all(copies, axis, split_axis=0, concat_axis=0, tiled=True)


def pack_x(core, x_weight, conv_weight, conv_bias):
    half = lax.dynamic_slice_in_dim(x_weight, core * 128, 128, 0)
    extra = jnp.concatenate([conv_weight, conv_bias[None, :], jnp.zeros((3, SHARD), BF16)], 0)
    return jnp.concatenate([half, jnp.pad(extra, ((0, 0), (0, 32)))], 0)


def pack_d(core, dt_weight, dt_bias, a_log, skip):
    half = lax.dynamic_slice_in_dim(dt_weight, core * 128, 128, 0)
    logs = lax.dynamic_slice_in_dim(a_log, core * 8, 8, 0)
    vec = jnp.where(core == 0, dt_bias, skip)[None, :]
    pieces = [half, *two_parts(logs), *two_parts(vec), jnp.zeros((6, SHARD), BF16)]
    return jnp.concatenate(pieces, 0)


def around(block, axis):
    up = [(i, (i + 1) % 4) for i in range(4)]
    down = [(i, (i - 1) % 4) for i in range(4)]
    previous = lax.ppermute(block, axis, up)
    following = lax.ppermute(block, axis, down)
    half = block.shape[0] // 2
    opposite = [lax.ppermute(previous[:half], axis, up), lax.ppermute(following[half:], axis, down)]
    return jnp.concatenate([block, following, *opposite, previous], 0).reshape(4, *block.shape)


def local(conv_input, gate_input, conv_weight, conv_bias, x_weight, dt_gain, dt_weight, dt_bias, a_log, skip):
    core = lax.axis_index("core")
    count = lax.axis_size(SEQ)
    swap = [(0, 1), (1, 0)]
    prior = lax.ppermute(conv_input[conv_input.shape[0] - 8 :], SEQ, [(i, i + 1) for i in range(count - 1)])
    x_part = from_everyone(pack_x(core, x_weight, conv_weight, conv_bias), "y")
    x_own = lax.all_gather(x_part[:, :128], "z", axis=0)
    params = x_part[:, 128:136, :SHARD].reshape(32, SHARD)
    d_part = from_everyone(jnp.concatenate([pack_d(core, dt_weight, dt_bias, a_log, skip), params], 0), "z")
    d_part = d_part.reshape(8, 184, SHARD)
    xc = conv(conv_input, prior, d_part[:, 152:].reshape(8, 4, 8, SHARD))
    d_own = around(d_part[:, :152], "y")
    d_oth = lax.ppermute(d_own, "core", swap)
    x_oth = lax.ppermute(x_own, "core", swap)
    where = jnp.stack([core, lax.axis_index("y")]).astype(jnp.int32)
    normed, bc = front(where, xc, x_own, x_oth, dt_gain[None, :])
    step, y, rate, ends = scan(where, normed, xc, d_own, d_oth, bc)
    ends = lax.all_to_all(ends, SEQ, split_axis=0, concat_axis=0, tiled=True)
    start = lax.all_to_all(link(ends, a_log), SEQ, split_axis=0, concat_axis=0, tiled=True)
    return close(step, y, rate, start, bc, gate_input)


def solution(mesh):
    inner = Mesh(mesh.devices.reshape(4, 8, 4, 2), ("y", "z", "x", "core"))
    tokens = P(("x", "core", "y", "z"), None)
    return jax.shard_map(
        local,
        mesh=inner,
        in_specs=(tokens, tokens, P(None, SEQ), P(SEQ), P(SEQ, None), P(), P(None, SEQ), P(SEQ), P(None, SEQ), P(SEQ)),
        out_specs=tokens,
        check_vma=False,
    )
```

```python
import jax
import jax.numpy as jnp
from jax import lax
from jax.experimental import pallas as pl
from jax.experimental.pallas import tpu as pltpu
from jax.sharding import Mesh, PartitionSpec as P

F32 = jnp.float32
BF16 = jnp.bfloat16
LOG2E = 1.4426950408889634
SEQ = ("y", "z")
BLK = 1024
SHARD = 256


def silu(v):
    return v / (1.0 + jnp.exp(-v))


def row_of(ref, at):
    return ref[pl.ds(at, 8, stride=0), :]


def two_parts(v):
    high = lax.reduce_precision(v, 8, 7)
    return high.astype(BF16), (v - high).astype(BF16)


def conv_kernel(ci_ref, prior_ref, par_ref, xc_ref, pad_ref):
    rows = ci_ref.shape[0]
    taps = 4
    pad_ref[0:8, :] = prior_ref[...].astype(F32)
    pad_ref[8 : 8 + rows, :] = ci_ref[...].astype(F32)
    for s in range(4):
        par = par_ref[0, s].astype(F32)
        lanes = slice(s * SHARD, (s + 1) * SHARD)
        total = jnp.broadcast_to(par[taps : taps + 1, :], (rows, SHARD))
        for k in range(taps):
            total = total + par[k : k + 1, :] * pad_ref[5 + k : 5 + k + rows, lanes]
        xc_ref[:, lanes] = silu(total).astype(BF16)


def conv(conv_input, prior, params):
    rows, inner = conv_input.shape
    return pl.pallas_call(
        conv_kernel,
        grid=(inner // BLK,),
        in_specs=[
            pl.BlockSpec((rows, BLK), lambda b: (0, b)),
            pl.BlockSpec((8, BLK), lambda b: (0, b)),
            pl.BlockSpec((1, 4, 8, SHARD), lambda b: (b // 2, b % 2, 0, 0)),
        ],
        out_specs=pl.BlockSpec((rows, BLK), lambda b: (0, b)),
        out_shape=jax.ShapeDtypeStruct((rows, inner), BF16),
        scratch_shapes=[pltpu.VMEM((rows + 8, BLK), F32)],
        compiler_params=pltpu.CompilerParams(dimension_semantics=("arbitrary",)),
        name="conv",
    )(conv_input, prior, params)


def times_rows(left, right):
    return lax.dot_general(left, right, (((1,), (1,)), ((), ())), preferred_element_type=F32)


def front_kernel(core_ref, xc_ref, own_ref, oth_ref, gain_ref, normed_ref, bc_ref, acc_ref):
    step = pl.program_id(0)
    core = core_ref[0]
    rows = xc_ref.shape[0]

    @pl.when(step == 0)
    def _():
        acc_ref[...] = jnp.zeros_like(acc_ref)

    acc = acc_ref[...]
    for s in range(4):
        at = pl.multiple_of(s * SHARD + core * 128, 128)
        acc = acc + times_rows(xc_ref[:, pl.ds(at, 128)], own_ref[s, 0])
        at = pl.multiple_of(s * SHARD + (1 - core) * 128, 128)
        acc = acc + times_rows(xc_ref[:, pl.ds(at, 128)], oth_ref[s, 0])
    acc_ref[...] = acc

    @pl.when(step == pl.num_programs(0) - 1)
    def _():
        rank = gain_ref.shape[1]
        low = acc_ref[:, 0:rank]
        scale = lax.rsqrt(jnp.mean(low * low, axis=1, keepdims=True) + 1e-06)
        normed_ref[...] = (low * scale * gain_ref[...]).astype(BF16)
        for m in range(32):
            col = acc_ref[:, rank + m : rank + m + 1]
            bc_ref[m * rows : (m + 1) * rows, :] = jnp.broadcast_to(col, (rows, 128))


def front(core, xc, x_own, x_oth, gain):
    rows, inner = xc.shape
    wspec = pl.BlockSpec((4, 1, 288, 128), lambda b: (b % 2, b // 2, 0, 0))
    return pl.pallas_call(
        front_kernel,
        grid=(inner // BLK,),
        in_specs=[
            pl.BlockSpec(memory_space=pltpu.SMEM),
            pl.BlockSpec((rows, BLK), lambda b: (0, b)),
            wspec,
            wspec,
            pl.BlockSpec((1, 256), lambda b: (0, 0)),
        ],
        out_specs=[
            pl.BlockSpec((rows, 256), lambda b: (0, 0)),
            pl.BlockSpec((32 * rows, 128), lambda b: (0, 0)),
        ],
        out_shape=[
            jax.ShapeDtypeStruct((rows, 256), BF16),
            jax.ShapeDtypeStruct((32 * rows, 128), F32),
        ],
        scratch_shapes=[pltpu.VMEM((rows, 288), F32)],
        compiler_params=pltpu.CompilerParams(dimension_semantics=("arbitrary",)),
        name="front",
    )(core, xc, x_own, x_oth, gain)


def scan_kernel(where_ref, normed_ref, xc_ref, own_ref, oth_ref, bc_ref, step_ref, y_ref, rate_ref, ends_ref, x_scr, par_scr, h_scr):
    core = where_ref[0]
    rows = normed_ref.shape[0]
    mine_k = normed_ref[:, pl.ds(pl.multiple_of(core * 128, 128), 128)]
    other_k = normed_ref[:, pl.ds(pl.multiple_of((1 - core) * 128, 128), 128)]
    skips = []
    for s in range(4):
        raw = jnp.dot(mine_k, own_ref[0, s, 0:128, :], preferred_element_type=F32)
        raw = raw + jnp.dot(other_k, oth_ref[0, s, 0:128, :], preferred_element_type=F32)
        mine = own_ref[0, s, 128:152, :].astype(F32)
        other = oth_ref[0, s, 128:152, :].astype(F32)
        mine_log = mine[0:8] + mine[8:16]
        other_log = other[0:8] + other[8:16]
        mine_vec = mine[16:17] + mine[17:18]
        other_vec = other[16:17] + other[17:18]
        bias = jnp.where(core == 0, mine_vec, other_vec)
        skip = jnp.where(core == 0, other_vec, mine_vec)
        raw = raw + bias
        step = jnp.maximum(raw, 0.0) + jnp.log1p(jnp.exp(-jnp.abs(raw)))
        xs = xc_ref[:, s * SHARD : (s + 1) * SHARD].astype(F32)
        for p in range(2):
            j = 2 * s + p
            lanes = slice(p * 128, (p + 1) * 128)
            for i in range(rows // 8):
                step_ref[0, pl.ds(64 * i + j, 8, stride=8), :] = step[8 * i : 8 * i + 8, lanes]
                x_scr[pl.ds(64 * i + j, 8, stride=8), :] = xs[8 * i : 8 * i + 8, lanes]
            at = pl.multiple_of(j * 16 + core * 8, 8)
            par_scr[pl.ds(at, 8), :] = -LOG2E * jnp.exp(mine_log[:, lanes])
            at = pl.multiple_of(j * 16 + (1 - core) * 8, 8)
            par_scr[pl.ds(at, 8), :] = -LOG2E * jnp.exp(other_log[:, lanes])
            skips.append(skip[:, lanes])
    skip = jnp.concatenate(skips, 0)
    for n in range(16):
        rate_ref[0, 8 * n : 8 * n + 8, :] = par_scr[pl.ds(n, 8, stride=16), :]
    rates = [rate_ref[0, 8 * n : 8 * n + 8, :] for n in range(16)]

    def advance(t, carry):
        total, state = carry
        at = pl.multiple_of(t * 8, 8)
        now = step_ref[0, pl.ds(at, 8), :]
        xt = x_scr[pl.ds(at, 8), :]
        drive = now * xt
        even = skip * xt
        odd = None
        fresh = []
        for n in range(16):
            b = row_of(bc_ref, n * rows + t)
            c = row_of(bc_ref, (16 + n) * rows + t)
            h = jnp.exp2(now * rates[n]) * state[n] + b * drive
            fresh.append(h)
            if n % 2:
                odd = c * h if odd is None else odd + c * h
            else:
                even = even + c * h
        y_ref[0, pl.ds(at, 8), :] = even + odd
        return total + now, tuple(fresh)

    zero = jnp.zeros((8, 128), F32)
    total, state = lax.fori_loop(0, rows, advance, (zero, (zero,) * 16), unroll=4)
    for n in range(16):
        h_scr[8 * n : 8 * n + 8, :] = state[n]
    high = total.astype(BF16).astype(F32)
    h_scr[128:136, :] = high
    h_scr[136:144, :] = total - high
    for j in range(8):
        low = h_scr[pl.ds(j, 8, stride=8), :]
        up = h_scr[pl.ds(64 + j, 8, stride=8), :]
        ends_ref[j // 2, (j % 2) * 16 : (j % 2) * 16 + 16, :] = jnp.concatenate([low, up], 0).astype(BF16)
    for jj in range(4):
        sums = [h_scr[128 + 2 * jj : 130 + 2 * jj, :], h_scr[136 + 2 * jj : 138 + 2 * jj, :], jnp.zeros((4, 128), F32)]
        ends_ref[jj, 32:40, :] = jnp.concatenate(sums, 0).astype(BF16)


def scan(where, normed, xc, d_own, d_oth, bc):
    rows, inner = xc.shape
    blocks = inner // BLK
    wspec = pl.BlockSpec((1, 4, 152, 256), lambda b, where: (b // 2, b % 2, 0, 0))
    grid_spec = pltpu.PrefetchScalarGridSpec(
        num_scalar_prefetch=1,
        grid=(blocks,),
        in_specs=[
            pl.BlockSpec((rows, 256), lambda b, where: (0, 0)),
            pl.BlockSpec((rows, BLK), lambda b, where: (0, b)),
            wspec,
            wspec,
            pl.BlockSpec((32 * rows, 128), lambda b, where: (0, 0)),
        ],
        out_specs=[
            pl.BlockSpec((1, 8 * rows, 128), lambda b, where: (b, 0, 0)),
            pl.BlockSpec((1, 8 * rows, 128), lambda b, where: (b, 0, 0)),
            pl.BlockSpec((1, 128, 128), lambda b, where: (b, 0, 0)),
            pl.BlockSpec((4, 40, 128), lambda b, where: (b, 0, 0)),
        ],
        scratch_shapes=[
            pltpu.VMEM((8 * rows, 128), F32),
            pltpu.VMEM((128, 128), F32),
            pltpu.VMEM((144, 128), F32),
        ],
    )
    return pl.pallas_call(
        scan_kernel,
        grid_spec=grid_spec,
        out_shape=[
            jax.ShapeDtypeStruct((blocks, 8 * rows, 128), F32),
            jax.ShapeDtypeStruct((blocks, 8 * rows, 128), F32),
            jax.ShapeDtypeStruct((blocks, 128, 128), F32),
            jax.ShapeDtypeStruct((4 * blocks, 40, 128), BF16),
        ],
        compiler_params=pltpu.CompilerParams(dimension_semantics=("arbitrary",)),
        name="scan",
    )(where, normed, xc, d_own, d_oth, bc)


def link_kernel(ends_ref, log_ref, start_ref):
    count = ends_ref.shape[0]
    rate = -LOG2E * jnp.exp(log_ref[...])
    rate = jnp.concatenate([rate[:, 0:128], rate[:, 128:256]], 0)
    state = jnp.zeros((32, 128), F32)
    for s in range(count):
        start_ref[s] = state.astype(BF16)
        sums = ends_ref[s, 32:40, :].astype(F32)
        sums = sums[0:2] + sums[2:4]
        spread = jnp.concatenate([jnp.broadcast_to(sums[0:1], (16, 128)), jnp.broadcast_to(sums[1:2], (16, 128))], 0)
        state = jnp.exp2(rate * spread) * state + ends_ref[s, 0:32, :].astype(F32)


def link(ends, a_log):
    return pl.pallas_call(
        link_kernel,
        out_shape=jax.ShapeDtypeStruct((ends.shape[0], 32, 128), BF16),
        name="link",
    )(ends, a_log)


def close_kernel(step_ref, y_ref, rate_ref, start_ref, c_ref, gate_ref, out_ref, s_scr, y_scr):
    rows = gate_ref.shape[0]
    for j in range(8):
        s_scr[16 * j : 16 * j + 16, :] = start_ref[j // 2, (j % 2) * 16 : (j % 2) * 16 + 16, :].astype(F32)
    starts = [s_scr[pl.ds(n, 8, stride=16), :] for n in range(16)]
    rates = [rate_ref[0, 8 * n : 8 * n + 8, :] for n in range(16)]

    def advance(t, total):
        at = pl.multiple_of(t * 8, 8)
        total = total + step_ref[0, pl.ds(at, 8), :]
        even = y_ref[0, pl.ds(at, 8), :]
        odd = None
        for n in range(16):
            c = row_of(c_ref, n * rows + t)
            part = c * starts[n] * jnp.exp2(total * rates[n])
            if n % 2:
                odd = part if odd is None else odd + part
            else:
                even = even + part
        y_scr[pl.ds(at, 8), :] = even + odd
        return total

    lax.fori_loop(0, rows, advance, jnp.zeros((8, 128), F32), unroll=4)
    for j in range(8):
        for i in range(rows // 16):
            low = y_scr[pl.ds(128 * i + j, 8, stride=8), :]
            up = y_scr[pl.ds(128 * i + 64 + j, 8, stride=8), :]
            y = jnp.concatenate([low, up], 0).astype(BF16).astype(F32)
            gate = gate_ref[16 * i : 16 * i + 16, j * 128 : (j + 1) * 128].astype(F32)
            out_ref[16 * i : 16 * i + 16, j * 128 : (j + 1) * 128] = (y * silu(gate)).astype(BF16)


def close(step, y, rate, start, bc, gate):
    rows, inner = gate.shape
    return pl.pallas_call(
        close_kernel,
        grid=(inner // BLK,),
        in_specs=[
            pl.BlockSpec((1, 8 * rows, 128), lambda b: (b, 0, 0)),
            pl.BlockSpec((1, 8 * rows, 128), lambda b: (b, 0, 0)),
            pl.BlockSpec((1, 128, 128), lambda b: (b, 0, 0)),
            pl.BlockSpec((4, 32, 128), lambda b: (b, 0, 0)),
            pl.BlockSpec((16 * rows, 128), lambda b: (1, 0)),
            pl.BlockSpec((rows, BLK), lambda b: (0, b)),
        ],
        out_specs=pl.BlockSpec((rows, BLK), lambda b: (0, b)),
        out_shape=jax.ShapeDtypeStruct((rows, inner), BF16),
        scratch_shapes=[pltpu.VMEM((128, 128), F32), pltpu.VMEM((8 * rows, 128), F32)],
        compiler_params=pltpu.CompilerParams(dimension_semantics=("arbitrary",)),
        name="close",
    )(step, y, rate, start, bc, gate)


def from_everyone(x, axis):
    copies = jnp.broadcast_to(x, (lax.axis_size(axis), *x.shape))
    return lax.all_to_all(copies, axis, split_axis=0, concat_axis=0, tiled=True)


def pack_x(core, x_weight):
    return lax.dynamic_slice_in_dim(x_weight.T, core * 128, 128, 1)


def pack_d(core, dt_weight, dt_bias, a_log, skip, conv_weight, conv_bias):
    half = lax.dynamic_slice_in_dim(dt_weight, core * 128, 128, 0)
    logs = lax.dynamic_slice_in_dim(a_log, core * 8, 8, 0)
    vec = jnp.where(core == 0, dt_bias, skip)[None, :]
    pieces = [half, *two_parts(logs), *two_parts(vec), jnp.zeros((6, SHARD), BF16)]
    pieces += [conv_weight, conv_bias[None, :], jnp.zeros((3, SHARD), BF16)]
    return jnp.concatenate(pieces, 0)


def shifted(block, axis, by):
    count = lax.axis_size(axis)
    return lax.ppermute(block, axis, [(i, (i + by) % count) for i in range(count)])


def placed(blocks, at, axis):
    count = lax.axis_size(axis)
    here = lax.axis_index(axis)
    first = blocks[0]
    out = jnp.zeros((count, *first.shape), first.dtype)
    for block, (by, row) in zip(blocks, at):
        out = lax.dynamic_update_slice(out, block[None], ((here + by) % count, row) + (0,) * (first.ndim - 1))
    return out


def together(*values):
    return lax.optimization_barrier(values)


def straight(block, axis):
    return [block] + [shifted(block, axis, k) for k in (1, 2, 3)], [(0, 0), (-1, 0), (-2, 0), (-3, 0)]


def local(conv_input, gate_input, conv_weight, conv_bias, x_weight, dt_gain, dt_weight, dt_bias, a_log, skip):
    core = lax.axis_index("core")
    count = lax.axis_size(SEQ)
    swap = [(0, 1), (1, 0)]
    prior = lax.ppermute(conv_input[conv_input.shape[0] - 8 :], SEQ, [(i, i + 1) for i in range(count - 1)])
    x_pieces, x_at = straight(pack_x(core, x_weight), "y")
    d_part = from_everyone(pack_d(core, dt_weight, dt_bias, a_log, skip, conv_weight, conv_bias), "z")
    x0 = placed(x_pieces, x_at, "y")
    x1 = shifted(x0, "z", 1), shifted(x0, "z", -1)
    *x1, d_part, prior = together(*x1, d_part, prior)
    d_part = d_part.reshape(8, 160, SHARD)
    d0 = d_part[:, :152]
    d1 = shifted(d0, "y", 1), shifted(d0, "y", -1)
    params = placed(*straight(d_part[:, 152:], "y"), "y")
    x2 = shifted(x1[0], "z", 1), shifted(x1[1], "z", -1)
    *x2, params = together(*x2, params)
    x3 = shifted(x2[0], "z", 1), shifted(x2[1], "z", -1)
    xc = conv(conv_input, prior, params)
    *x3, xc, up, down = together(*x3, xc, *d1)
    d1 = up, down
    x4 = shifted(x3[0][:2], "z", 1), shifted(x3[1][2:], "z", -1)
    d2 = shifted(d1[0][:4], "y", 1), shifted(d1[1][4:], "y", -1)
    x_own = placed([x0, *x1, *x2, *x3, *x4], [(0, 0), (-1, 0), (1, 0), (-2, 0), (2, 0), (-3, 0), (3, 0), (4, 0), (4, 2)], "z")
    x_oth = lax.ppermute(x_own, "core", swap)
    d_own = placed([d0, *d1, *d2], [(0, 0), (-1, 0), (1, 0), (2, 0), (2, 4)], "y")
    d_oth = lax.ppermute(d_own, "core", swap)
    where = jnp.stack([core, core]).astype(jnp.int32)
    normed, bc = front(where, xc, x_own, x_oth, dt_gain[None, :])
    step, y, rate, ends = scan(where, normed, xc, d_own, d_oth, bc)
    ends = lax.all_to_all(ends, SEQ, split_axis=0, concat_axis=0, tiled=True)
    start = lax.all_to_all(link(ends, a_log), SEQ, split_axis=0, concat_axis=0, tiled=True)
    return close(step, y, rate, start, bc, gate_input)


def solution(mesh):
    inner = Mesh(mesh.devices.reshape(4, 8, 4, 2), ("y", "z", "x", "core"))
    tokens = P(("x", "core", "y", "z"), None)
    return jax.shard_map(
        local,
        mesh=inner,
        in_specs=(tokens, tokens, P(None, SEQ), P(SEQ), P(SEQ, None), P(), P(None, SEQ), P(SEQ), P(None, SEQ), P(SEQ)),
        out_specs=tokens,
        check_vma=False,
    )
```

```python
import jax
import jax.numpy as jnp
from jax import lax
from jax.experimental import pallas as pl
from jax.experimental.pallas import tpu as pltpu
from jax.sharding import Mesh, PartitionSpec as P

F32 = jnp.float32
BF16 = jnp.bfloat16
LOG2E = 1.4426950408889634
SEQ = ("y", "z")
BLK = 1024
SHARD = 256


def silu(v):
    return v / (1.0 + jnp.exp(-v))


def row_of(ref, at):
    return ref[pl.ds(at, 8, stride=0), :]


def two_parts(v):
    high = lax.reduce_precision(v, 8, 7)
    return high.astype(BF16), (v - high).astype(BF16)


def conv_kernel(ci_ref, prior_ref, par_ref, xc_ref, pad_ref):
    rows = ci_ref.shape[0]
    taps = 4
    pad_ref[0:8, :] = prior_ref[...].astype(F32)
    pad_ref[8 : 8 + rows, :] = ci_ref[...].astype(F32)
    for s in range(4):
        par = jnp.concatenate([par_ref[s, 0:8, :], par_ref[s, 8:16, :]], 1).astype(F32)
        lanes = slice(s * SHARD, (s + 1) * SHARD)
        total = jnp.broadcast_to(par[taps : taps + 1, :], (rows, SHARD))
        for k in range(taps):
            total = total + par[k : k + 1, :] * pad_ref[5 + k : 5 + k + rows, lanes]
        xc_ref[:, lanes] = silu(total).astype(BF16)


def conv(conv_input, prior, params):
    rows, inner = conv_input.shape
    return pl.pallas_call(
        conv_kernel,
        grid=(inner // BLK,),
        in_specs=[
            pl.BlockSpec((rows, BLK), lambda b: (0, b)),
            pl.BlockSpec((8, BLK), lambda b: (0, b)),
            pl.BlockSpec((4, 16, 128), lambda b: (b, 0, 0)),
        ],
        out_specs=pl.BlockSpec((rows, BLK), lambda b: (0, b)),
        out_shape=jax.ShapeDtypeStruct((rows, inner), BF16),
        scratch_shapes=[pltpu.VMEM((rows + 8, BLK), F32)],
        compiler_params=pltpu.CompilerParams(dimension_semantics=("arbitrary",)),
        name="conv",
    )(conv_input, prior, params)


def times_rows(left, right):
    return lax.dot_general(left, right, (((1,), (1,)), ((), ())), preferred_element_type=F32)


def front_kernel(core_ref, xc_ref, own_ref, oth_ref, gain_ref, normed_ref, bc_ref, acc_ref):
    core = core_ref[0]
    rows = xc_ref.shape[0]
    rank = gain_ref.shape[1]
    acc_ref[...] = jnp.zeros_like(acc_ref)

    def add_shards(group, _):
        acc = acc_ref[...]
        for k in range(4):
            s = group * 4 + k
            mine = pl.multiple_of(s * SHARD + core * 128, 128)
            other = pl.multiple_of(s * SHARD + (1 - core) * 128, 128)
            left = jnp.concatenate([xc_ref[:, pl.ds(mine, 128)], xc_ref[:, pl.ds(other, 128)]], 1)
            right = [jnp.concatenate([ref[q, s] for q in range(4)], 0) for ref in (own_ref, oth_ref)]
            acc = acc + times_rows(left, jnp.concatenate(right, 1))
        acc_ref[...] = acc
        return 0

    lax.fori_loop(0, own_ref.shape[1] // 4, add_shards, 0)
    low = acc_ref[:, 0:rank]
    scale = lax.rsqrt(jnp.mean(low * low, axis=1, keepdims=True) + 1e-06)
    normed_ref[...] = (low * scale * gain_ref[...]).astype(BF16)
    for m in range(32):
        col = acc_ref[:, rank + m : rank + m + 1]
        bc_ref[m * rows : (m + 1) * rows, :] = jnp.broadcast_to(col, (rows, 128))


def front(core, xc, x_own, x_oth, gain):
    rows = xc.shape[0]
    vmem = pl.BlockSpec(memory_space=pltpu.VMEM)
    return pl.pallas_call(
        front_kernel,
        in_specs=[pl.BlockSpec(memory_space=pltpu.SMEM), vmem, vmem, vmem, vmem],
        out_specs=[vmem, vmem],
        out_shape=[
            jax.ShapeDtypeStruct((rows, 256), BF16),
            jax.ShapeDtypeStruct((32 * rows, 128), F32),
        ],
        scratch_shapes=[pltpu.VMEM((rows, 320), F32)],
        name="front",
    )(core, xc, x_own, x_oth, gain)


def scan_kernel(where_ref, normed_ref, xc_ref, own_ref, oth_ref, bc_ref, step_ref, y_ref, rate_ref, ends_ref, x_scr, par_scr, h_scr):
    core = where_ref[0]
    rows = normed_ref.shape[0]
    mine_k = normed_ref[:, pl.ds(pl.multiple_of(core * 128, 128), 128)]
    other_k = normed_ref[:, pl.ds(pl.multiple_of((1 - core) * 128, 128), 128)]
    skips = []
    for s in range(4):
        raw = jnp.dot(mine_k, own_ref[0, s, 0:128, :], preferred_element_type=F32)
        raw = raw + jnp.dot(other_k, oth_ref[0, s, 0:128, :], preferred_element_type=F32)
        mine = own_ref[0, s, 128:152, :].astype(F32)
        other = oth_ref[0, s, 128:152, :].astype(F32)
        mine_log = mine[0:8] + mine[8:16]
        other_log = other[0:8] + other[8:16]
        mine_vec = mine[16:17] + mine[17:18]
        other_vec = other[16:17] + other[17:18]
        bias = jnp.where(core == 0, mine_vec, other_vec)
        skip = jnp.where(core == 0, other_vec, mine_vec)
        raw = raw + bias
        step = jnp.maximum(raw, 0.0) + jnp.log1p(jnp.exp(-jnp.abs(raw)))
        xs = xc_ref[:, s * SHARD : (s + 1) * SHARD].astype(F32)
        for p in range(2):
            j = 2 * s + p
            lanes = slice(p * 128, (p + 1) * 128)
            for i in range(rows // 8):
                step_ref[0, pl.ds(64 * i + j, 8, stride=8), :] = step[8 * i : 8 * i + 8, lanes]
                x_scr[pl.ds(64 * i + j, 8, stride=8), :] = xs[8 * i : 8 * i + 8, lanes]
            at = pl.multiple_of(j * 16 + core * 8, 8)
            par_scr[pl.ds(at, 8), :] = -LOG2E * jnp.exp(mine_log[:, lanes])
            at = pl.multiple_of(j * 16 + (1 - core) * 8, 8)
            par_scr[pl.ds(at, 8), :] = -LOG2E * jnp.exp(other_log[:, lanes])
            skips.append(skip[:, lanes])
    skip = jnp.concatenate(skips, 0)
    for n in range(16):
        rate_ref[0, 8 * n : 8 * n + 8, :] = par_scr[pl.ds(n, 8, stride=16), :]
    rates = [rate_ref[0, 8 * n : 8 * n + 8, :] for n in range(16)]

    def advance(t, carry):
        total, state = carry
        at = pl.multiple_of(t * 8, 8)
        now = step_ref[0, pl.ds(at, 8), :]
        xt = x_scr[pl.ds(at, 8), :]
        drive = now * xt
        even = skip * xt
        odd = None
        fresh = []
        for n in range(16):
            b = row_of(bc_ref, n * rows + t)
            c = row_of(bc_ref, (16 + n) * rows + t)
            h = jnp.exp2(now * rates[n]) * state[n] + b * drive
            fresh.append(h)
            if n % 2:
                odd = c * h if odd is None else odd + c * h
            else:
                even = even + c * h
        y_ref[0, pl.ds(at, 8), :] = even + odd
        return total + now, tuple(fresh)

    zero = jnp.zeros((8, 128), F32)
    total, state = lax.fori_loop(0, rows, advance, (zero, (zero,) * 16), unroll=4)
    for n in range(16):
        h_scr[8 * n : 8 * n + 8, :] = state[n]
    high = total.astype(BF16).astype(F32)
    h_scr[128:136, :] = high
    h_scr[136:144, :] = total - high
    for j in range(8):
        low = h_scr[pl.ds(j, 8, stride=8), :]
        up = h_scr[pl.ds(64 + j, 8, stride=8), :]
        ends_ref[j // 2, (j % 2) * 16 : (j % 2) * 16 + 16, :] = jnp.concatenate([low, up], 0).astype(BF16)
    for jj in range(4):
        sums = [h_scr[128 + 2 * jj : 130 + 2 * jj, :], h_scr[136 + 2 * jj : 138 + 2 * jj, :], jnp.zeros((4, 128), F32)]
        ends_ref[jj, 32:40, :] = jnp.concatenate(sums, 0).astype(BF16)


def scan(where, normed, xc, d_own, d_oth, bc):
    rows, inner = xc.shape
    blocks = inner // BLK
    wspec = pl.BlockSpec((1, 4, 152, 256), lambda b, where: (b // 2, b % 2, 0, 0))
    grid_spec = pltpu.PrefetchScalarGridSpec(
        num_scalar_prefetch=1,
        grid=(blocks,),
        in_specs=[
            pl.BlockSpec((rows, 256), lambda b, where: (0, 0)),
            pl.BlockSpec((rows, BLK), lambda b, where: (0, b)),
            wspec,
            wspec,
            pl.BlockSpec((32 * rows, 128), lambda b, where: (0, 0)),
        ],
        out_specs=[
            pl.BlockSpec((1, 8 * rows, 128), lambda b, where: (b, 0, 0)),
            pl.BlockSpec((1, 8 * rows, 128), lambda b, where: (b, 0, 0)),
            pl.BlockSpec((1, 128, 128), lambda b, where: (b, 0, 0)),
            pl.BlockSpec((4, 40, 128), lambda b, where: (b, 0, 0)),
        ],
        scratch_shapes=[
            pltpu.VMEM((8 * rows, 128), F32),
            pltpu.VMEM((128, 128), F32),
            pltpu.VMEM((144, 128), F32),
        ],
    )
    return pl.pallas_call(
        scan_kernel,
        grid_spec=grid_spec,
        out_shape=[
            jax.ShapeDtypeStruct((blocks, 8 * rows, 128), F32),
            jax.ShapeDtypeStruct((blocks, 8 * rows, 128), F32),
            jax.ShapeDtypeStruct((blocks, 128, 128), F32),
            jax.ShapeDtypeStruct((4 * blocks, 40, 128), BF16),
        ],
        compiler_params=pltpu.CompilerParams(dimension_semantics=("arbitrary",)),
        name="scan",
    )(where, normed, xc, d_own, d_oth, bc)


def link_kernel(ends_ref, log_ref, start_ref):
    count = ends_ref.shape[0]
    rate = -LOG2E * jnp.exp(log_ref[...])
    rate = jnp.concatenate([rate[:, 0:128], rate[:, 128:256]], 0)
    state = jnp.zeros((32, 128), F32)
    for s in range(count):
        start_ref[s] = state.astype(BF16)
        sums = ends_ref[s, 32:40, :].astype(F32)
        sums = sums[0:2] + sums[2:4]
        spread = jnp.concatenate([jnp.broadcast_to(sums[0:1], (16, 128)), jnp.broadcast_to(sums[1:2], (16, 128))], 0)
        state = jnp.exp2(rate * spread) * state + ends_ref[s, 0:32, :].astype(F32)


def link(ends, a_log):
    return pl.pallas_call(
        link_kernel,
        out_shape=jax.ShapeDtypeStruct((ends.shape[0], 32, 128), BF16),
        name="link",
    )(ends, a_log)


def close_kernel(step_ref, y_ref, rate_ref, start_ref, c_ref, gate_ref, out_ref, s_scr, y_scr):
    rows = gate_ref.shape[0]
    for j in range(8):
        s_scr[16 * j : 16 * j + 16, :] = start_ref[j // 2, (j % 2) * 16 : (j % 2) * 16 + 16, :].astype(F32)
    starts = [s_scr[pl.ds(n, 8, stride=16), :] for n in range(16)]
    rates = [rate_ref[0, 8 * n : 8 * n + 8, :] for n in range(16)]

    def advance(t, total):
        at = pl.multiple_of(t * 8, 8)
        total = total + step_ref[0, pl.ds(at, 8), :]
        even = y_ref[0, pl.ds(at, 8), :]
        odd = None
        for n in range(16):
            c = row_of(c_ref, n * rows + t)
            part = c * starts[n] * jnp.exp2(total * rates[n])
            if n % 2:
                odd = part if odd is None else odd + part
            else:
                even = even + part
        y_scr[pl.ds(at, 8), :] = even + odd
        return total

    lax.fori_loop(0, rows, advance, jnp.zeros((8, 128), F32), unroll=4)
    for j in range(8):
        for i in range(rows // 16):
            low = y_scr[pl.ds(128 * i + j, 8, stride=8), :]
            up = y_scr[pl.ds(128 * i + 64 + j, 8, stride=8), :]
            y = jnp.concatenate([low, up], 0).astype(BF16).astype(F32)
            gate = gate_ref[16 * i : 16 * i + 16, j * 128 : (j + 1) * 128].astype(F32)
            out_ref[16 * i : 16 * i + 16, j * 128 : (j + 1) * 128] = (y * silu(gate)).astype(BF16)


def close(step, y, rate, start, bc, gate):
    rows, inner = gate.shape
    return pl.pallas_call(
        close_kernel,
        grid=(inner // BLK,),
        in_specs=[
            pl.BlockSpec((1, 8 * rows, 128), lambda b: (b, 0, 0)),
            pl.BlockSpec((1, 8 * rows, 128), lambda b: (b, 0, 0)),
            pl.BlockSpec((1, 128, 128), lambda b: (b, 0, 0)),
            pl.BlockSpec((4, 32, 128), lambda b: (b, 0, 0)),
            pl.BlockSpec((16 * rows, 128), lambda b: (1, 0)),
            pl.BlockSpec((rows, BLK), lambda b: (0, b)),
        ],
        out_specs=pl.BlockSpec((rows, BLK), lambda b: (0, b)),
        out_shape=jax.ShapeDtypeStruct((rows, inner), BF16),
        scratch_shapes=[pltpu.VMEM((128, 128), F32), pltpu.VMEM((8 * rows, 128), F32)],
        compiler_params=pltpu.CompilerParams(dimension_semantics=("arbitrary",)),
        name="close",
    )(step, y, rate, start, bc, gate)


def from_everyone(x, axis):
    copies = jnp.broadcast_to(x, (lax.axis_size(axis), *x.shape))
    return lax.all_to_all(copies, axis, split_axis=0, concat_axis=0, tiled=True)


def pack_x(core, quarter, x_weight, conv_weight, conv_bias):
    half = lax.dynamic_slice_in_dim(x_weight.T, core * 128, 128, 1)
    part = lax.dynamic_slice_in_dim(jnp.pad(half, ((0, 32), (0, 0))), quarter * 80, 80, 0)
    taps = jnp.concatenate([conv_weight, conv_bias[None, :], jnp.zeros((3, SHARD), BF16)], 0)
    return jnp.concatenate([part, taps[:, :128], taps[:, 128:]], 0)


def pack_d(core, dt_weight, dt_bias, a_log, skip):
    half = lax.dynamic_slice_in_dim(dt_weight, core * 128, 128, 0)
    logs = lax.dynamic_slice_in_dim(a_log, core * 8, 8, 0)
    vec = jnp.where(core == 0, dt_bias, skip)[None, :]
    pieces = [half, *two_parts(logs), *two_parts(vec), jnp.zeros((6, SHARD), BF16)]
    return jnp.concatenate(pieces, 0)


def shifted(block, axis, by):
    count = lax.axis_size(axis)
    return lax.ppermute(block, axis, [(i, (i + by) % count) for i in range(count)])


def placed(blocks, at, axis):
    count = lax.axis_size(axis)
    here = lax.axis_index(axis)
    first = blocks[0]
    out = jnp.zeros((count, *first.shape), first.dtype)
    for block, (by, row) in zip(blocks, at):
        out = lax.dynamic_update_slice(out, block[None], ((here + by) % count, row) + (0,) * (first.ndim - 1))
    return out


def together(*values):
    return lax.optimization_barrier(values)


def around_eight(block, axis):
    near = {k: shifted(block, axis, -k) for k in (1, -1, 2, -2)}
    near = dict(zip(near, together(*near.values())))
    far = {3: shifted(near[2], axis, -1), -3: shifted(near[-2], axis, 1), 4: shifted(near[-2], axis, 2)}
    blocks = {0: block, **near, **far}
    return placed(list(blocks.values()), [(k, 0) for k in blocks], axis)


def halves_on(up, down, axis):
    half = up.shape[0] // 2
    return shifted(up[:half], axis, 1), shifted(down[half:], axis, -1)


def around_four(block, first, second, axis):
    half = block.shape[0] // 2
    return placed([block, *first, *second], [(0, 0), (-1, 0), (1, 0), (2, 0), (2, half)], axis)


def local(conv_input, gate_input, conv_weight, conv_bias, x_weight, dt_gain, dt_weight, dt_bias, a_log, skip):
    core = lax.axis_index("core")
    count = lax.axis_size(SEQ)
    swap = [(0, 1), (1, 0)]
    prior = lax.ppermute(conv_input[conv_input.shape[0] - 8 :], SEQ, [(i, i + 1) for i in range(count - 1)])
    x_part = from_everyone(pack_x(core, lax.axis_index("x"), x_weight, conv_weight, conv_bias)[None], SEQ)
    d0 = around_eight(pack_d(core, dt_weight, dt_bias, a_log, skip), "z")
    x_part, d0, prior = together(x_part, d0, prior)
    x_part = x_part.reshape(count, 96, 128)
    x0 = x_part[:, :80]
    x1 = shifted(x0, "x", 1), shifted(x0, "x", -1)
    d1 = shifted(d0, "y", 1), shifted(d0, "y", -1)
    xc = conv(conv_input, prior, x_part[:, 80:])
    *x1, xc = together(*x1, xc)
    x2 = halves_on(*x1, "x")
    d2 = halves_on(*d1, "y")
    x_own = around_four(x0, x1, x2, "x")
    x_oth = lax.ppermute(x_own, "core", swap)
    d_own = around_four(d0, d1, d2, "y")
    d_oth = lax.ppermute(d_own, "core", swap)
    where = core.reshape(1).astype(jnp.int32)
    normed, bc = front(where, xc, x_own, x_oth, dt_gain[None, :])
    step, y, rate, ends = scan(where, normed, xc, d_own, d_oth, bc)
    ends = lax.all_to_all(ends, SEQ, split_axis=0, concat_axis=0, tiled=True)
    start = lax.all_to_all(link(ends, a_log), SEQ, split_axis=0, concat_axis=0, tiled=True)
    return close(step, y, rate, start, bc, gate_input)


def solution(mesh):
    inner = Mesh(mesh.devices.reshape(4, 8, 4, 2), ("y", "z", "x", "core"))
    tokens = P(("x", "core", "y", "z"), None)
    return jax.shard_map(
        local,
        mesh=inner,
        in_specs=(tokens, tokens, P(None, SEQ), P(SEQ), P(SEQ, None), P(), P(None, SEQ), P(SEQ), P(None, SEQ), P(SEQ)),
        out_specs=tokens,
        check_vma=False,
    )
```

```python
import jax
import jax.numpy as jnp
from jax import lax
from jax.experimental import pallas as pl
from jax.experimental.pallas import tpu as pltpu
from jax.sharding import Mesh, PartitionSpec as P


F32 = jnp.float32
BF16 = jnp.bfloat16
LOG2E = 1.4426950408889634
SEQ = ("y", "z")
BLK = 1024
SHARD = 256


def silu(v):
    return v / (1.0 + jnp.exp(-v))


def row_of(ref, at):
    return ref[pl.ds(at, 8, stride=0), :]


def two_parts(v):
    high = lax.reduce_precision(v, 8, 7)
    return high.astype(BF16), (v - high).astype(BF16)


def conv_kernel(core_ref, ci_ref, prior_ref, par_ref, xc_ref, lend_ref, pad_ref):
    core = core_ref[0]
    rows = ci_ref.shape[0]
    taps = 4
    pad_ref[0:8, :] = prior_ref[...].astype(F32)
    pad_ref[8 : 8 + rows, :] = ci_ref[...].astype(F32)
    for s in range(4):
        par = par_ref[s, 0].astype(F32)
        lanes = slice(s * SHARD, (s + 1) * SHARD)
        total = jnp.broadcast_to(par[taps : taps + 1, :], (rows, SHARD))
        for k in range(taps):
            total = total + par[k : k + 1, :] * pad_ref[5 + k : 5 + k + rows, lanes]
        xc_ref[:, lanes] = silu(total).astype(BF16)
        at = pl.multiple_of(s * SHARD + (1 - core) * 128, 128)
        lend_ref[:, s * 128 : (s + 1) * 128] = xc_ref[:, pl.ds(at, 128)]


def conv(core, conv_input, prior, params):
    rows, inner = conv_input.shape
    return pl.pallas_call(
        conv_kernel,
        grid=(inner // BLK,),
        in_specs=[
            pl.BlockSpec(memory_space=pltpu.SMEM),
            pl.BlockSpec((rows, BLK), lambda b: (0, b)),
            pl.BlockSpec((8, BLK), lambda b: (0, b)),
            pl.BlockSpec((4, 1, 8, SHARD), lambda b: (b % 2, b // 2, 0, 0)),
        ],
        out_specs=[
            pl.BlockSpec((rows, BLK), lambda b: (0, b)),
            pl.BlockSpec((rows, BLK // 2), lambda b: (0, b)),
        ],
        out_shape=[
            jax.ShapeDtypeStruct((rows, inner), BF16),
            jax.ShapeDtypeStruct((rows, inner // 2), BF16),
        ],
        scratch_shapes=[pltpu.VMEM((rows + 8, BLK), F32)],
        compiler_params=pltpu.CompilerParams(dimension_semantics=("arbitrary",)),
        name="conv",
    )(core, conv_input, prior, params)


AWAY = (0, -1, 1, -2, 2, -3, 3, 4, 4)


def times_rows(left, right):
    return lax.dot_general(left, right, (((1,), (1,)), ((), ())), preferred_element_type=F32)


def project_kernel(where_ref, xc_ref, lent_ref, *refs):
    blocks, (own_ref, other_ref) = refs[:-2], refs[-2:]
    core, here = where_ref[0], where_ref[1]
    rows = xc_ref.shape[0]
    total = None
    for k, (away, block) in enumerate(zip(AWAY, blocks)):
        first = 2 if k == len(AWAY) - 1 else 0
        z = lax.rem(here + 8 + away, 8)
        for row in range(0, block.shape[0], 2):
            left = []
            for y in (first + row, first + row + 1):
                mine = pl.multiple_of((y * 8 + z) * SHARD + core * 128, 128)
                lent = pl.multiple_of((y * 8 + z) * 128, 128)
                left.append(jnp.concatenate([xc_ref[:, pl.ds(mine, 128)], lent_ref[:, pl.ds(lent, 128)]], 0))
            right = jnp.concatenate([block[row, 0:288, :], block[row + 1, 0:288, :]], 1)
            part = times_rows(jnp.concatenate(left, 1), right)
            total = part if total is None else total + part
    own_ref[...] = total[:rows]
    other_ref[...] = total[rows:]


def project(where, xc, lent, blocks):
    rows = xc.shape[0]
    vmem = pl.BlockSpec(memory_space=pltpu.VMEM)
    shape = jax.ShapeDtypeStruct((rows, 288), F32)
    return pl.pallas_call(
        project_kernel,
        in_specs=[pl.BlockSpec(memory_space=pltpu.SMEM)] + [vmem] * (2 + len(blocks)),
        out_specs=[vmem, vmem],
        out_shape=[shape, shape],
        name="project",
    )(where, xc, lent, *blocks)


def norm_kernel(own_ref, other_ref, gain_ref, normed_ref, bc_ref):
    rows, rank = normed_ref.shape
    proj = own_ref[...] + other_ref[...]
    low = proj[:, 0:rank]
    scale = lax.rsqrt(jnp.mean(low * low, axis=1, keepdims=True) + 1e-06)
    normed_ref[...] = (low * scale * gain_ref[...]).astype(BF16)
    for m in range(32):
        bc_ref[m * rows : (m + 1) * rows, :] = jnp.broadcast_to(proj[:, rank + m : rank + m + 1], (rows, 128))


def norm(own, other, gain):
    rows = own.shape[0]
    vmem = pl.BlockSpec(memory_space=pltpu.VMEM)
    return pl.pallas_call(
        norm_kernel,
        in_specs=[vmem, vmem, vmem],
        out_specs=[vmem, vmem],
        out_shape=[
            jax.ShapeDtypeStruct((rows, 256), BF16),
            jax.ShapeDtypeStruct((32 * rows, 128), F32),
        ],
        name="norm",
    )(own, other, gain)


def scan_kernel(where_ref, normed_ref, xc_ref, own_ref, oth_ref, bc_ref, step_ref, y_ref, rate_ref, ends_ref, x_scr, par_scr, h_scr):
    core = where_ref[0]
    rows = normed_ref.shape[0]
    mine_k = normed_ref[:, pl.ds(pl.multiple_of(core * 128, 128), 128)]
    other_k = normed_ref[:, pl.ds(pl.multiple_of((1 - core) * 128, 128), 128)]
    skips = []
    for s in range(4):
        raw = jnp.dot(mine_k, own_ref[0, s, 0:128, :], preferred_element_type=F32)
        raw = raw + jnp.dot(other_k, oth_ref[0, s, 0:128, :], preferred_element_type=F32)
        mine = own_ref[0, s, 128:152, :].astype(F32)
        other = oth_ref[0, s, 128:152, :].astype(F32)
        mine_log = mine[0:8] + mine[8:16]
        other_log = other[0:8] + other[8:16]
        mine_vec = mine[16:17] + mine[17:18]
        other_vec = other[16:17] + other[17:18]
        bias = jnp.where(core == 0, mine_vec, other_vec)
        skip = jnp.where(core == 0, other_vec, mine_vec)
        raw = raw + bias
        step = jnp.maximum(raw, 0.0) + jnp.log1p(jnp.exp(-jnp.abs(raw)))
        xs = xc_ref[:, s * SHARD : (s + 1) * SHARD].astype(F32)
        for p in range(2):
            j = 2 * s + p
            lanes = slice(p * 128, (p + 1) * 128)
            for i in range(rows // 8):
                step_ref[0, pl.ds(64 * i + j, 8, stride=8), :] = step[8 * i : 8 * i + 8, lanes]
                x_scr[pl.ds(64 * i + j, 8, stride=8), :] = xs[8 * i : 8 * i + 8, lanes]
            at = pl.multiple_of(j * 16 + core * 8, 8)
            par_scr[pl.ds(at, 8), :] = -LOG2E * jnp.exp(mine_log[:, lanes])
            at = pl.multiple_of(j * 16 + (1 - core) * 8, 8)
            par_scr[pl.ds(at, 8), :] = -LOG2E * jnp.exp(other_log[:, lanes])
            skips.append(skip[:, lanes])
    skip = jnp.concatenate(skips, 0)
    for n in range(16):
        rate_ref[0, 8 * n : 8 * n + 8, :] = par_scr[pl.ds(n, 8, stride=16), :]
    rates = [rate_ref[0, 8 * n : 8 * n + 8, :] for n in range(16)]

    def advance(t, carry):
        total, state = carry
        at = pl.multiple_of(t * 8, 8)
        now = step_ref[0, pl.ds(at, 8), :]
        xt = x_scr[pl.ds(at, 8), :]
        drive = now * xt
        even = skip * xt
        odd = None
        fresh = []
        for n in range(16):
            b = row_of(bc_ref, n * rows + t)
            c = row_of(bc_ref, (16 + n) * rows + t)
            h = jnp.exp2(now * rates[n]) * state[n] + b * drive
            fresh.append(h)
            if n % 2:
                odd = c * h if odd is None else odd + c * h
            else:
                even = even + c * h
        y_ref[0, pl.ds(at, 8), :] = even + odd
        return total + now, tuple(fresh)

    zero = jnp.zeros((8, 128), F32)
    total, state = lax.fori_loop(0, rows, advance, (zero, (zero,) * 16), unroll=4)
    for n in range(16):
        h_scr[8 * n : 8 * n + 8, :] = state[n]
    high = total.astype(BF16).astype(F32)
    h_scr[128:136, :] = high
    h_scr[136:144, :] = total - high
    for j in range(8):
        low = h_scr[pl.ds(j, 8, stride=8), :]
        up = h_scr[pl.ds(64 + j, 8, stride=8), :]
        ends_ref[j // 2, (j % 2) * 16 : (j % 2) * 16 + 16, :] = jnp.concatenate([low, up], 0).astype(BF16)
    for jj in range(4):
        sums = [h_scr[128 + 2 * jj : 130 + 2 * jj, :], h_scr[136 + 2 * jj : 138 + 2 * jj, :], jnp.zeros((4, 128), F32)]
        ends_ref[jj, 32:40, :] = jnp.concatenate(sums, 0).astype(BF16)


def scan(where, normed, xc, d_own, d_oth, bc):
    rows, inner = xc.shape
    blocks = inner // BLK
    wspec = pl.BlockSpec((1, 4, 152, 256), lambda b, where: (b // 2, b % 2, 0, 0))
    grid_spec = pltpu.PrefetchScalarGridSpec(
        num_scalar_prefetch=1,
        grid=(blocks,),
        in_specs=[
            pl.BlockSpec((rows, 256), lambda b, where: (0, 0)),
            pl.BlockSpec((rows, BLK), lambda b, where: (0, b)),
            wspec,
            wspec,
            pl.BlockSpec((32 * rows, 128), lambda b, where: (0, 0)),
        ],
        out_specs=[
            pl.BlockSpec((1, 8 * rows, 128), lambda b, where: (b, 0, 0)),
            pl.BlockSpec((1, 8 * rows, 128), lambda b, where: (b, 0, 0)),
            pl.BlockSpec((1, 128, 128), lambda b, where: (b, 0, 0)),
            pl.BlockSpec((4, 40, 128), lambda b, where: (b, 0, 0)),
        ],
        scratch_shapes=[
            pltpu.VMEM((8 * rows, 128), F32),
            pltpu.VMEM((128, 128), F32),
            pltpu.VMEM((144, 128), F32),
        ],
    )
    return pl.pallas_call(
        scan_kernel,
        grid_spec=grid_spec,
        out_shape=[
            jax.ShapeDtypeStruct((blocks, 8 * rows, 128), F32),
            jax.ShapeDtypeStruct((blocks, 8 * rows, 128), F32),
            jax.ShapeDtypeStruct((blocks, 128, 128), F32),
            jax.ShapeDtypeStruct((4 * blocks, 40, 128), BF16),
        ],
        compiler_params=pltpu.CompilerParams(dimension_semantics=("arbitrary",)),
        name="scan",
    )(where, normed, xc, d_own, d_oth, bc)


def link_kernel(ends_ref, log_ref, start_ref):
    count = ends_ref.shape[0]
    rate = -LOG2E * jnp.exp(log_ref[...])
    rate = jnp.concatenate([rate[:, 0:128], rate[:, 128:256]], 0)
    state = jnp.zeros((32, 128), F32)
    for s in range(count):
        start_ref[s] = state.astype(BF16)
        sums = ends_ref[s, 32:40, :].astype(F32)
        sums = sums[0:2] + sums[2:4]
        spread = jnp.concatenate([jnp.broadcast_to(sums[0:1], (16, 128)), jnp.broadcast_to(sums[1:2], (16, 128))], 0)
        state = jnp.exp2(rate * spread) * state + ends_ref[s, 0:32, :].astype(F32)


def link(ends, a_log):
    return pl.pallas_call(
        link_kernel,
        out_shape=jax.ShapeDtypeStruct((ends.shape[0], 32, 128), BF16),
        name="link",
    )(ends, a_log)


def close_kernel(step_ref, y_ref, rate_ref, start_ref, c_ref, gate_ref, out_ref, s_scr, y_scr):
    rows = gate_ref.shape[0]
    for j in range(8):
        s_scr[16 * j : 16 * j + 16, :] = start_ref[j // 2, (j % 2) * 16 : (j % 2) * 16 + 16, :].astype(F32)
    starts = [s_scr[pl.ds(n, 8, stride=16), :] for n in range(16)]
    rates = [rate_ref[0, 8 * n : 8 * n + 8, :] for n in range(16)]

    def advance(t, total):
        at = pl.multiple_of(t * 8, 8)
        total = total + step_ref[0, pl.ds(at, 8), :]
        even = y_ref[0, pl.ds(at, 8), :]
        odd = None
        for n in range(16):
            c = row_of(c_ref, n * rows + t)
            part = c * starts[n] * jnp.exp2(total * rates[n])
            if n % 2:
                odd = part if odd is None else odd + part
            else:
                even = even + part
        y_scr[pl.ds(at, 8), :] = even + odd
        return total

    lax.fori_loop(0, rows, advance, jnp.zeros((8, 128), F32), unroll=4)
    for j in range(8):
        for i in range(rows // 16):
            low = y_scr[pl.ds(128 * i + j, 8, stride=8), :]
            up = y_scr[pl.ds(128 * i + 64 + j, 8, stride=8), :]
            y = jnp.concatenate([low, up], 0).astype(BF16).astype(F32)
            gate = gate_ref[16 * i : 16 * i + 16, j * 128 : (j + 1) * 128].astype(F32)
            out_ref[16 * i : 16 * i + 16, j * 128 : (j + 1) * 128] = (y * silu(gate)).astype(BF16)


def close(step, y, rate, start, bc, gate):
    rows, inner = gate.shape
    return pl.pallas_call(
        close_kernel,
        grid=(inner // BLK,),
        in_specs=[
            pl.BlockSpec((1, 8 * rows, 128), lambda b: (b, 0, 0)),
            pl.BlockSpec((1, 8 * rows, 128), lambda b: (b, 0, 0)),
            pl.BlockSpec((1, 128, 128), lambda b: (b, 0, 0)),
            pl.BlockSpec((4, 32, 128), lambda b: (b, 0, 0)),
            pl.BlockSpec((16 * rows, 128), lambda b: (1, 0)),
            pl.BlockSpec((rows, BLK), lambda b: (0, b)),
        ],
        out_specs=pl.BlockSpec((rows, BLK), lambda b: (0, b)),
        out_shape=jax.ShapeDtypeStruct((rows, inner), BF16),
        scratch_shapes=[pltpu.VMEM((128, 128), F32), pltpu.VMEM((8 * rows, 128), F32)],
        compiler_params=pltpu.CompilerParams(dimension_semantics=("arbitrary",)),
        name="close",
    )(step, y, rate, start, bc, gate)


def from_everyone(x, axis):
    copies = jnp.broadcast_to(x, (lax.axis_size(axis), *x.shape))
    return lax.all_to_all(copies, axis, split_axis=0, concat_axis=0, tiled=True)


def pack_x(core, x_weight, conv_weight, conv_bias):
    half = lax.dynamic_slice_in_dim(x_weight.T, core * 128, 128, 1)
    taps = jnp.concatenate([conv_weight, conv_bias[None, :], jnp.zeros((3, SHARD), BF16)], 0)
    return jnp.concatenate([half, taps[:, :128], taps[:, 128:]], 0)


def pack_d(core, dt_weight, dt_bias, a_log, skip):
    half = lax.dynamic_slice_in_dim(dt_weight, core * 128, 128, 0)
    logs = lax.dynamic_slice_in_dim(a_log, core * 8, 8, 0)
    vec = jnp.where(core == 0, dt_bias, skip)[None, :]
    pieces = [half, *two_parts(logs), *two_parts(vec), jnp.zeros((6, SHARD), BF16)]
    return jnp.concatenate(pieces, 0)


def shifted(block, axis, by):
    count = lax.axis_size(axis)
    return lax.ppermute(block, axis, [(i, (i + by) % count) for i in range(count)])


def placed(blocks, at, axis):
    count = lax.axis_size(axis)
    here = lax.axis_index(axis)
    first = blocks[0]
    out = jnp.zeros((count, *first.shape), first.dtype)
    for block, (by, row) in zip(blocks, at):
        out = lax.dynamic_update_slice(out, block[None], ((here + by) % count, row) + (0,) * (first.ndim - 1))
    return out


def together(*values):
    return lax.optimization_barrier(values)


def both_ways(pair, axis):
    return shifted(pair[0], axis, 1), shifted(pair[1], axis, -1)


def body(conv_input, gate_input, conv_weight, conv_bias, x_weight, dt_gain, dt_weight, dt_bias, a_log, skip):
    core = lax.axis_index("core")
    count = lax.axis_size(SEQ)
    swap = [(0, 1), (1, 0)]
    where = jnp.stack([core, lax.axis_index("z")]).astype(jnp.int32)
    prior = lax.ppermute(conv_input[conv_input.shape[0] - 8 :], SEQ, [(i, i + 1) for i in range(count - 1)])
    x_piece = pack_x(core, x_weight, conv_weight, conv_bias)
    x_pieces = [x_piece] + [shifted(x_piece, "y", k) for k in (1, 2, 3)]
    x0 = placed(x_pieces, [(0, 0), (-1, 0), (-2, 0), (-3, 0)], "y")
    x1 = both_ways((x0, x0), "z")
    taps = jnp.concatenate([x0[:, 288:296], x0[:, 296:304]], 2).reshape(32, SHARD)
    d_msg = jnp.concatenate([pack_d(core, dt_weight, dt_bias, a_log, skip), taps], 0)
    d_part = from_everyone(d_msg, "z").reshape(8, 184, SHARD)
    x2 = both_ways(x1, "z")
    *x2, d_part, prior = together(*x2, d_part, prior)
    d0 = d_part[:, :152]
    d1 = both_ways((d0, d0), "y")
    x3 = both_ways(x2, "z")
    xc, lend = conv(where, conv_input, prior, d_part[:, 152:].reshape(8, 4, 8, SHARD))
    lent = lax.ppermute(lend, "core", swap)
    *x3, xc, up, down = together(*x3, xc, *d1)
    x4 = both_ways((x3[0][:2], x3[1][2:]), "z")
    d2 = both_ways((up[:4], down[4:]), "y")
    d_own = placed([d0, up, down, *d2], [(0, 0), (-1, 0), (1, 0), (2, 0), (2, 4)], "y")
    d_oth = lax.ppermute(d_own, "core", swap)
    own, other = project(where, xc, lent, [x0, *x1, *x2, *x3, *x4])
    normed, bc = norm(own, lax.ppermute(other, "core", swap), dt_gain[None, :])
    step, y, rate, ends = scan(where, normed, xc, d_own, d_oth, bc)
    ends = lax.all_to_all(ends, SEQ, split_axis=0, concat_axis=0, tiled=True)
    start = lax.all_to_all(link(ends, a_log), SEQ, split_axis=0, concat_axis=0, tiled=True)
    return close(step, y, rate, start, bc, gate_input)


def solution(mesh):
    inner = Mesh(mesh.devices.reshape(4, 8, 4, 2), ("y", "z", "x", "core"))
    tokens = P(("x", "core", "y", "z"), None)
    return jax.shard_map(
        body,
        mesh=inner,
        in_specs=(tokens, tokens, P(None, SEQ), P(SEQ), P(SEQ, None), P(), P(None, SEQ), P(SEQ), P(None, SEQ), P(SEQ)),
        out_specs=tokens,
        check_vma=False,
    )
```

```python
import jax
import jax.numpy as jnp
from jax import lax
from jax.experimental import pallas as pl
from jax.experimental.pallas import tpu as pltpu
from jax.sharding import Mesh, PartitionSpec as P


F32 = jnp.float32
BF16 = jnp.bfloat16
LOG2E = 1.4426950408889634
SEQ = ("y", "z")
BLK = 1024
SHARD = 256


def silu(v):
    return v / (1.0 + jnp.exp(-v))


def row_of(ref, at):
    return ref[pl.ds(at, 8, stride=0), :]


def two_parts(v):
    high = lax.reduce_precision(v, 8, 7)
    return high.astype(BF16), (v - high).astype(BF16)


def conv_kernel(core_ref, ci_ref, prior_ref, par_ref, xc_ref, lend_ref, pad_ref):
    core = core_ref[0]
    rows = ci_ref.shape[0]
    taps = 4
    pad_ref[0:8, :] = prior_ref[...].astype(F32)
    pad_ref[8 : 8 + rows, :] = ci_ref[...].astype(F32)
    for s in range(4):
        par = par_ref[s, 0].astype(F32)
        lanes = slice(s * SHARD, (s + 1) * SHARD)
        total = jnp.broadcast_to(par[taps : taps + 1, :], (rows, SHARD))
        for k in range(taps):
            total = total + par[k : k + 1, :] * pad_ref[5 + k : 5 + k + rows, lanes]
        xc_ref[:, lanes] = silu(total).astype(BF16)
        at = pl.multiple_of(s * SHARD + (1 - core) * 128, 128)
        lend_ref[:, s * 128 : (s + 1) * 128] = xc_ref[:, pl.ds(at, 128)]


def conv(core, conv_input, prior, params):
    rows, inner = conv_input.shape
    return pl.pallas_call(
        conv_kernel,
        grid=(inner // BLK,),
        in_specs=[
            pl.BlockSpec(memory_space=pltpu.SMEM),
            pl.BlockSpec((rows, BLK), lambda b: (0, b)),
            pl.BlockSpec((8, BLK), lambda b: (0, b)),
            pl.BlockSpec((4, 1, 8, SHARD), lambda b: (b % 2, b // 2, 0, 0)),
        ],
        out_specs=[
            pl.BlockSpec((rows, BLK), lambda b: (0, b)),
            pl.BlockSpec((rows, BLK // 2), lambda b: (0, b)),
        ],
        out_shape=[
            jax.ShapeDtypeStruct((rows, inner), BF16),
            jax.ShapeDtypeStruct((rows, inner // 2), BF16),
        ],
        scratch_shapes=[pltpu.VMEM((rows + 8, BLK), F32)],
        compiler_params=pltpu.CompilerParams(dimension_semantics=("arbitrary",)),
        name="conv",
    )(core, conv_input, prior, params)


AWAY = (0, -1, 1, -2, 2, -3, 3, 4, 4)


def times_rows(left, right):
    return lax.dot_general(left, right, (((1,), (1,)), ((), ())), preferred_element_type=F32)


def project_kernel(where_ref, xc_ref, lent_ref, *refs):
    blocks, (own_ref, other_ref) = refs[:-2], refs[-2:]
    core, here = where_ref[0], where_ref[1]
    rows = xc_ref.shape[0]
    total = None
    for k, (away, block) in enumerate(zip(AWAY, blocks)):
        first = 2 if k == len(AWAY) - 1 else 0
        z = lax.rem(here + 8 + away, 8)
        for row in range(0, block.shape[0], 2):
            left = []
            for y in (first + row, first + row + 1):
                mine = pl.multiple_of((y * 8 + z) * SHARD + core * 128, 128)
                lent = pl.multiple_of((y * 8 + z) * 128, 128)
                left.append(jnp.concatenate([xc_ref[:, pl.ds(mine, 128)], lent_ref[:, pl.ds(lent, 128)]], 0))
            right = jnp.concatenate([block[row, 0:288, :], block[row + 1, 0:288, :]], 1)
            part = times_rows(jnp.concatenate(left, 1), right)
            total = part if total is None else total + part
    own_ref[...] = total[:rows]
    other_ref[...] = total[rows:]


def project(where, xc, lent, blocks):
    rows = xc.shape[0]
    vmem = pl.BlockSpec(memory_space=pltpu.VMEM)
    shape = jax.ShapeDtypeStruct((rows, 288), F32)
    return pl.pallas_call(
        project_kernel,
        in_specs=[pl.BlockSpec(memory_space=pltpu.SMEM)] + [vmem] * (2 + len(blocks)),
        out_specs=[vmem, vmem],
        out_shape=[shape, shape],
        name="project",
    )(where, xc, lent, *blocks)


def norm_kernel(own_ref, other_ref, gain_ref, normed_ref, bc_ref):
    rows, rank = normed_ref.shape
    proj = own_ref[...] + other_ref[...]
    low = proj[:, 0:rank]
    scale = lax.rsqrt(jnp.mean(low * low, axis=1, keepdims=True) + 1e-06)
    normed_ref[...] = (low * scale * gain_ref[...]).astype(BF16)
    for m in range(32):
        bc_ref[m * rows : (m + 1) * rows, :] = jnp.broadcast_to(proj[:, rank + m : rank + m + 1], (rows, 128))


def norm(own, other, gain):
    rows = own.shape[0]
    vmem = pl.BlockSpec(memory_space=pltpu.VMEM)
    return pl.pallas_call(
        norm_kernel,
        in_specs=[vmem, vmem, vmem],
        out_specs=[vmem, vmem],
        out_shape=[
            jax.ShapeDtypeStruct((rows, 256), BF16),
            jax.ShapeDtypeStruct((32 * rows, 128), F32),
        ],
        name="norm",
    )(own, other, gain)


def scan_kernel(where_ref, normed_ref, xc_ref, own_ref, oth_ref, bc_ref, step_ref, y_ref, rate_ref, ends_ref, x_scr, par_scr, h_scr):
    core = where_ref[0]
    rows = normed_ref.shape[0]
    mine_k = normed_ref[:, pl.ds(pl.multiple_of(core * 128, 128), 128)]
    other_k = normed_ref[:, pl.ds(pl.multiple_of((1 - core) * 128, 128), 128)]
    skips = []
    for s in range(4):
        raw = jnp.dot(mine_k, own_ref[0, s, 0:128, :], preferred_element_type=F32)
        raw = raw + jnp.dot(other_k, oth_ref[0, s, 0:128, :], preferred_element_type=F32)
        mine = own_ref[0, s, 128:152, :].astype(F32)
        other = oth_ref[0, s, 128:152, :].astype(F32)
        mine_log = mine[0:8] + mine[8:16]
        other_log = other[0:8] + other[8:16]
        mine_vec = mine[16:17] + mine[17:18]
        other_vec = other[16:17] + other[17:18]
        bias = jnp.where(core == 0, mine_vec, other_vec)
        skip = jnp.where(core == 0, other_vec, mine_vec)
        raw = raw + bias
        step = jnp.maximum(raw, 0.0) + jnp.log1p(jnp.exp(-jnp.abs(raw)))
        xs = xc_ref[:, s * SHARD : (s + 1) * SHARD].astype(F32)
        for p in range(2):
            j = 2 * s + p
            lanes = slice(p * 128, (p + 1) * 128)
            for i in range(rows // 8):
                step_ref[0, pl.ds(64 * i + j, 8, stride=8), :] = step[8 * i : 8 * i + 8, lanes]
                x_scr[pl.ds(64 * i + j, 8, stride=8), :] = xs[8 * i : 8 * i + 8, lanes]
            at = pl.multiple_of(j * 16 + core * 8, 8)
            par_scr[pl.ds(at, 8), :] = -LOG2E * jnp.exp(mine_log[:, lanes])
            at = pl.multiple_of(j * 16 + (1 - core) * 8, 8)
            par_scr[pl.ds(at, 8), :] = -LOG2E * jnp.exp(other_log[:, lanes])
            skips.append(skip[:, lanes])
    skip = jnp.concatenate(skips, 0)
    for n in range(16):
        rate_ref[0, 8 * n : 8 * n + 8, :] = par_scr[pl.ds(n, 8, stride=16), :]
    rates = [rate_ref[0, 8 * n : 8 * n + 8, :] for n in range(16)]

    def advance(t, carry):
        total, state = carry
        at = pl.multiple_of(t * 8, 8)
        now = step_ref[0, pl.ds(at, 8), :]
        xt = x_scr[pl.ds(at, 8), :]
        drive = now * xt
        even = skip * xt
        odd = None
        fresh = []
        for n in range(16):
            b = row_of(bc_ref, n * rows + t)
            c = row_of(bc_ref, (16 + n) * rows + t)
            h = jnp.exp2(now * rates[n]) * state[n] + b * drive
            fresh.append(h)
            if n % 2:
                odd = c * h if odd is None else odd + c * h
            else:
                even = even + c * h
        y_ref[0, pl.ds(at, 8), :] = even + odd
        return total + now, tuple(fresh)

    zero = jnp.zeros((8, 128), F32)
    total, state = lax.fori_loop(0, rows, advance, (zero, (zero,) * 16), unroll=8)
    for n in range(16):
        h_scr[8 * n : 8 * n + 8, :] = state[n]
    high = total.astype(BF16).astype(F32)
    h_scr[128:136, :] = high
    h_scr[136:144, :] = total - high
    for j in range(8):
        low = h_scr[pl.ds(j, 8, stride=8), :]
        up = h_scr[pl.ds(64 + j, 8, stride=8), :]
        ends_ref[j // 2, (j % 2) * 16 : (j % 2) * 16 + 16, :] = jnp.concatenate([low, up], 0).astype(BF16)
    for jj in range(4):
        sums = [h_scr[128 + 2 * jj : 130 + 2 * jj, :], h_scr[136 + 2 * jj : 138 + 2 * jj, :], jnp.zeros((4, 128), F32)]
        ends_ref[jj, 32:40, :] = jnp.concatenate(sums, 0).astype(BF16)


def scan(where, normed, xc, d_own, d_oth, bc):
    rows, inner = xc.shape
    blocks = inner // BLK
    wspec = pl.BlockSpec((1, 4, 152, 256), lambda b, where: (b // 2, b % 2, 0, 0))
    grid_spec = pltpu.PrefetchScalarGridSpec(
        num_scalar_prefetch=1,
        grid=(blocks,),
        in_specs=[
            pl.BlockSpec((rows, 256), lambda b, where: (0, 0)),
            pl.BlockSpec((rows, BLK), lambda b, where: (0, b)),
            wspec,
            wspec,
            pl.BlockSpec((32 * rows, 128), lambda b, where: (0, 0)),
        ],
        out_specs=[
            pl.BlockSpec((1, 8 * rows, 128), lambda b, where: (b, 0, 0)),
            pl.BlockSpec((1, 8 * rows, 128), lambda b, where: (b, 0, 0)),
            pl.BlockSpec((1, 128, 128), lambda b, where: (b, 0, 0)),
            pl.BlockSpec((4, 40, 128), lambda b, where: (b, 0, 0)),
        ],
        scratch_shapes=[
            pltpu.VMEM((8 * rows, 128), F32),
            pltpu.VMEM((128, 128), F32),
            pltpu.VMEM((144, 128), F32),
        ],
    )
    return pl.pallas_call(
        scan_kernel,
        grid_spec=grid_spec,
        out_shape=[
            jax.ShapeDtypeStruct((blocks, 8 * rows, 128), F32),
            jax.ShapeDtypeStruct((blocks, 8 * rows, 128), F32),
            jax.ShapeDtypeStruct((blocks, 128, 128), F32),
            jax.ShapeDtypeStruct((4 * blocks, 40, 128), BF16),
        ],
        compiler_params=pltpu.CompilerParams(dimension_semantics=("arbitrary",)),
        name="scan",
    )(where, normed, xc, d_own, d_oth, bc)


def link_kernel(ends_ref, log_ref, start_ref):
    count = ends_ref.shape[0]
    rate = -LOG2E * jnp.exp(log_ref[...])
    rate = jnp.concatenate([rate[:, 0:128], rate[:, 128:256]], 0)
    state = jnp.zeros((32, 128), F32)
    for s in range(count):
        start_ref[s] = state.astype(BF16)
        sums = ends_ref[s, 32:40, :].astype(F32)
        sums = sums[0:2] + sums[2:4]
        spread = jnp.concatenate([jnp.broadcast_to(sums[0:1], (16, 128)), jnp.broadcast_to(sums[1:2], (16, 128))], 0)
        state = jnp.exp2(rate * spread) * state + ends_ref[s, 0:32, :].astype(F32)


def link(ends, a_log):
    return pl.pallas_call(
        link_kernel,
        out_shape=jax.ShapeDtypeStruct((ends.shape[0], 32, 128), BF16),
        name="link",
    )(ends, a_log)


def close_kernel(step_ref, y_ref, rate_ref, start_ref, c_ref, gate_ref, out_ref, s_scr, y_scr):
    rows = gate_ref.shape[0]
    for j in range(8):
        s_scr[16 * j : 16 * j + 16, :] = start_ref[j // 2, (j % 2) * 16 : (j % 2) * 16 + 16, :].astype(F32)
    starts = [s_scr[pl.ds(n, 8, stride=16), :] for n in range(16)]
    rates = [rate_ref[0, 8 * n : 8 * n + 8, :] for n in range(16)]

    def advance(t, total):
        at = pl.multiple_of(t * 8, 8)
        total = total + step_ref[0, pl.ds(at, 8), :]
        even = y_ref[0, pl.ds(at, 8), :]
        odd = None
        for n in range(16):
            c = row_of(c_ref, n * rows + t)
            part = c * starts[n] * jnp.exp2(total * rates[n])
            if n % 2:
                odd = part if odd is None else odd + part
            else:
                even = even + part
        y_scr[pl.ds(at, 8), :] = even + odd
        return total

    lax.fori_loop(0, rows, advance, jnp.zeros((8, 128), F32), unroll=8)
    for j in range(8):
        for i in range(rows // 16):
            low = y_scr[pl.ds(128 * i + j, 8, stride=8), :]
            up = y_scr[pl.ds(128 * i + 64 + j, 8, stride=8), :]
            y = jnp.concatenate([low, up], 0).astype(BF16).astype(F32)
            gate = gate_ref[16 * i : 16 * i + 16, j * 128 : (j + 1) * 128].astype(F32)
            out_ref[16 * i : 16 * i + 16, j * 128 : (j + 1) * 128] = (y * silu(gate)).astype(BF16)


def close(step, y, rate, start, bc, gate):
    rows, inner = gate.shape
    return pl.pallas_call(
        close_kernel,
        grid=(inner // BLK,),
        in_specs=[
            pl.BlockSpec((1, 8 * rows, 128), lambda b: (b, 0, 0)),
            pl.BlockSpec((1, 8 * rows, 128), lambda b: (b, 0, 0)),
            pl.BlockSpec((1, 128, 128), lambda b: (b, 0, 0)),
            pl.BlockSpec((4, 32, 128), lambda b: (b, 0, 0)),
            pl.BlockSpec((16 * rows, 128), lambda b: (1, 0)),
            pl.BlockSpec((rows, BLK), lambda b: (0, b)),
        ],
        out_specs=pl.BlockSpec((rows, BLK), lambda b: (0, b)),
        out_shape=jax.ShapeDtypeStruct((rows, inner), BF16),
        scratch_shapes=[pltpu.VMEM((128, 128), F32), pltpu.VMEM((8 * rows, 128), F32)],
        compiler_params=pltpu.CompilerParams(dimension_semantics=("arbitrary",)),
        name="close",
    )(step, y, rate, start, bc, gate)


def from_everyone(x, axis):
    copies = jnp.broadcast_to(x, (lax.axis_size(axis), *x.shape))
    return lax.all_to_all(copies, axis, split_axis=0, concat_axis=0, tiled=True)


def pack_x(core, x_weight, conv_weight, conv_bias):
    half = lax.dynamic_slice_in_dim(x_weight.T, core * 128, 128, 1)
    taps = jnp.concatenate([conv_weight, conv_bias[None, :], jnp.zeros((3, SHARD), BF16)], 0)
    return jnp.concatenate([half, taps[:, :128], taps[:, 128:]], 0)


def pack_d(core, dt_weight, dt_bias, a_log, skip):
    half = lax.dynamic_slice_in_dim(dt_weight, core * 128, 128, 0)
    logs = lax.dynamic_slice_in_dim(a_log, core * 8, 8, 0)
    vec = jnp.where(core == 0, dt_bias, skip)[None, :]
    pieces = [half, *two_parts(logs), *two_parts(vec), jnp.zeros((6, SHARD), BF16)]
    return jnp.concatenate(pieces, 0)


def shifted(block, axis, by):
    count = lax.axis_size(axis)
    return lax.ppermute(block, axis, [(i, (i + by) % count) for i in range(count)])


def placed(blocks, at, axis):
    count = lax.axis_size(axis)
    here = lax.axis_index(axis)
    first = blocks[0]
    out = jnp.zeros((count, *first.shape), first.dtype)
    for block, (by, row) in zip(blocks, at):
        out = lax.dynamic_update_slice(out, block[None], ((here + by) % count, row) + (0,) * (first.ndim - 1))
    return out


def together(*values):
    return lax.optimization_barrier(values)


def both_ways(pair, axis):
    return shifted(pair[0], axis, 1), shifted(pair[1], axis, -1)


def body(conv_input, gate_input, conv_weight, conv_bias, x_weight, dt_gain, dt_weight, dt_bias, a_log, skip):
    core = lax.axis_index("core")
    count = lax.axis_size(SEQ)
    swap = [(0, 1), (1, 0)]
    where = jnp.stack([core, lax.axis_index("z")]).astype(jnp.int32)
    prior = lax.ppermute(conv_input[conv_input.shape[0] - 8 :], SEQ, [(i, i + 1) for i in range(count - 1)])
    x_piece = pack_x(core, x_weight, conv_weight, conv_bias)
    x_pieces = [x_piece] + [shifted(x_piece, "y", k) for k in (1, 2, 3)]
    x0 = placed(x_pieces, [(0, 0), (-1, 0), (-2, 0), (-3, 0)], "y")
    x1 = both_ways((x0, x0), "z")
    taps = jnp.concatenate([x0[:, 288:296], x0[:, 296:304]], 2).reshape(32, SHARD)
    d_msg = jnp.concatenate([pack_d(core, dt_weight, dt_bias, a_log, skip), taps], 0)
    d_part = from_everyone(d_msg, "z").reshape(8, 184, SHARD)
    x2 = both_ways(x1, "z")
    d0 = d_part[:, :152]
    d1 = both_ways((d0, d0), "y")
    x3 = both_ways(x2, "z")
    xc, lend = conv(where, conv_input, prior, d_part[:, 152:].reshape(8, 4, 8, SHARD))
    *x3, xc, lend = together(*x3, xc, lend)
    up, down = d1
    lent = lax.ppermute(lend, "core", swap)
    x4 = both_ways((x3[0][:2], x3[1][2:]), "z")
    d2 = both_ways((up[:4], down[4:]), "y")
    d_own = placed([d0, up, down, *d2], [(0, 0), (-1, 0), (1, 0), (2, 0), (2, 4)], "y")
    d_oth = lax.ppermute(d_own, "core", swap)
    own, other = project(where, xc, lent, [x0, *x1, *x2, *x3, *x4])
    other = lax.ppermute(other, "core", swap)
    normed, bc = norm(own, other, dt_gain[None, :])
    step, y, rate, ends = scan(where, normed, xc, d_own, d_oth, bc)
    ends = lax.all_to_all(ends, SEQ, split_axis=0, concat_axis=0, tiled=True)
    start = lax.all_to_all(link(ends, a_log), SEQ, split_axis=0, concat_axis=0, tiled=True)
    return close(step, y, rate, start, bc, gate_input)


def solution(mesh):
    inner = Mesh(mesh.devices.reshape(4, 8, 4, 2), ("y", "z", "x", "core"))
    tokens = P(("x", "core", "y", "z"), None)
    return jax.shard_map(
        body,
        mesh=inner,
        in_specs=(tokens, tokens, P(None, SEQ), P(SEQ), P(SEQ, None), P(), P(None, SEQ), P(SEQ), P(None, SEQ), P(SEQ)),
        out_specs=tokens,
        check_vma=False,
    )
```

```python
import jax
import jax.numpy as jnp
from jax import lax
from jax.experimental import pallas as pl
from jax.experimental.pallas import tpu as pltpu
from jax.sharding import Mesh, PartitionSpec as P


F32 = jnp.float32
BF16 = jnp.bfloat16
LOG2E = 1.4426950408889634
SEQ = ("y", "z")
BLK = 1024
SHARD = 256


def silu(v):
    return v / (1.0 + jnp.exp(-v))


def row_of(ref, at):
    return ref[pl.ds(at, 8, stride=0), :]


def two_parts(v):
    high = lax.reduce_precision(v, 8, 7)
    return high.astype(BF16), (v - high).astype(BF16)


def conv_kernel(core_ref, ci_ref, prior_ref, par_ref, xc_ref, lend_ref, pad_ref):
    core = core_ref[0]
    rows = ci_ref.shape[0]
    taps = 4
    pad_ref[0:8, :] = prior_ref[...].astype(F32)
    pad_ref[8 : 8 + rows, :] = ci_ref[...].astype(F32)
    for s in range(4):
        par = par_ref[0, s].astype(F32)
        lanes = slice(s * SHARD, (s + 1) * SHARD)
        total = jnp.broadcast_to(par[taps : taps + 1, :], (rows, SHARD))
        for k in range(taps):
            total = total + par[k : k + 1, :] * pad_ref[5 + k : 5 + k + rows, lanes]
        xc_ref[:, lanes] = silu(total).astype(BF16)
        at = pl.multiple_of(s * SHARD + (1 - core) * 128, 128)
        lend_ref[:, s * 128 : (s + 1) * 128] = xc_ref[:, pl.ds(at, 128)]


def conv(core, conv_input, prior, params):
    rows, inner = conv_input.shape
    return pl.pallas_call(
        conv_kernel,
        grid=(inner // BLK,),
        in_specs=[
            pl.BlockSpec(memory_space=pltpu.SMEM),
            pl.BlockSpec((rows, BLK), lambda b: (0, b)),
            pl.BlockSpec((8, BLK), lambda b: (0, b)),
            pl.BlockSpec((1, 4, 8, SHARD), lambda b: (b // 2, b % 2, 0, 0)),
        ],
        out_specs=[
            pl.BlockSpec((rows, BLK), lambda b: (0, b)),
            pl.BlockSpec((rows, BLK // 2), lambda b: (0, b)),
        ],
        out_shape=[
            jax.ShapeDtypeStruct((rows, inner), BF16),
            jax.ShapeDtypeStruct((rows, inner // 2), BF16),
        ],
        scratch_shapes=[pltpu.VMEM((rows + 8, BLK), F32)],
        compiler_params=pltpu.CompilerParams(dimension_semantics=("arbitrary",)),
        name="conv",
    )(core, conv_input, prior, params)


AWAY = (0, -1, 1, -2, 2, -3, 3, 4, 4)


def times_rows(left, right):
    return lax.dot_general(left, right, (((1,), (1,)), ((), ())), preferred_element_type=F32)


def project_kernel(where_ref, xc_ref, lent_ref, *refs):
    blocks, (own_ref, other_ref) = refs[:-2], refs[-2:]
    core, here = where_ref[0], where_ref[1]
    rows = xc_ref.shape[0]
    total = None
    for k, (away, block) in enumerate(zip(AWAY, blocks)):
        first = 2 if k == len(AWAY) - 1 else 0
        z = lax.rem(here + 8 + away, 8)
        for row in range(0, block.shape[0], 2):
            left = []
            for y in (first + row, first + row + 1):
                mine = pl.multiple_of((y * 8 + z) * SHARD + core * 128, 128)
                lent = pl.multiple_of((y * 8 + z) * 128, 128)
                left.append(jnp.concatenate([xc_ref[:, pl.ds(mine, 128)], lent_ref[:, pl.ds(lent, 128)]], 0))
            right = jnp.concatenate([block[row, 0:288, :], block[row + 1, 0:288, :]], 1)
            part = times_rows(jnp.concatenate(left, 1), right)
            total = part if total is None else total + part
    own_ref[...] = total[:rows]
    other_ref[...] = total[rows:]


def project(where, xc, lent, blocks):
    rows = xc.shape[0]
    vmem = pl.BlockSpec(memory_space=pltpu.VMEM)
    shape = jax.ShapeDtypeStruct((rows, 288), F32)
    return pl.pallas_call(
        project_kernel,
        in_specs=[pl.BlockSpec(memory_space=pltpu.SMEM)] + [vmem] * (2 + len(blocks)),
        out_specs=[vmem, vmem],
        out_shape=[shape, shape],
        name="project",
    )(where, xc, lent, *blocks)


def spread(proj, first, count, out_ref):
    rows = proj.shape[0]
    for m in range(count):
        out_ref[m * rows : (m + 1) * rows, :] = jnp.broadcast_to(proj[:, first + m : first + m + 1], (rows, 128))


def scan_kernel(where_ref, mine_ref, other_ref, gain_ref, xc_ref, own_ref, oth_ref, step_ref, y_ref, rate_ref, ends_ref, *scratch):
    x_scr, par_scr, h_scr, normed_ref, bc_ref = scratch
    core = where_ref[0]
    rows = xc_ref.shape[0]
    rank = gain_ref.shape[1]

    @pl.when(pl.program_id(0) == 0)
    def _():
        proj = mine_ref[...] + other_ref[...]
        low = proj[:, 0:rank]
        scale = lax.rsqrt(jnp.mean(low * low, axis=1, keepdims=True) + 1e-06)
        normed_ref[...] = (low * scale * gain_ref[...]).astype(BF16)
        spread(proj, rank, 32, bc_ref)

    mine_k = normed_ref[:, pl.ds(pl.multiple_of(core * 128, 128), 128)]
    other_k = normed_ref[:, pl.ds(pl.multiple_of((1 - core) * 128, 128), 128)]
    skips = []
    for s in range(4):
        raw = jnp.dot(mine_k, own_ref[0, s, 0:128, :], preferred_element_type=F32)
        raw = raw + jnp.dot(other_k, oth_ref[0, s, 0:128, :], preferred_element_type=F32)
        mine = own_ref[0, s, 128:152, :].astype(F32)
        other = oth_ref[0, s, 128:152, :].astype(F32)
        mine_log = mine[0:8] + mine[8:16]
        other_log = other[0:8] + other[8:16]
        mine_vec = mine[16:17] + mine[17:18]
        other_vec = other[16:17] + other[17:18]
        bias = jnp.where(core == 0, mine_vec, other_vec)
        skip = jnp.where(core == 0, other_vec, mine_vec)
        raw = raw + bias
        step = jnp.maximum(raw, 0.0) + jnp.log1p(jnp.exp(-jnp.abs(raw)))
        xs = xc_ref[:, s * SHARD : (s + 1) * SHARD].astype(F32)
        for p in range(2):
            j = 2 * s + p
            lanes = slice(p * 128, (p + 1) * 128)
            for i in range(rows // 8):
                step_ref[0, pl.ds(64 * i + j, 8, stride=8), :] = step[8 * i : 8 * i + 8, lanes]
                x_scr[pl.ds(64 * i + j, 8, stride=8), :] = xs[8 * i : 8 * i + 8, lanes]
            at = pl.multiple_of(j * 16 + core * 8, 8)
            par_scr[pl.ds(at, 8), :] = -LOG2E * jnp.exp(mine_log[:, lanes])
            at = pl.multiple_of(j * 16 + (1 - core) * 8, 8)
            par_scr[pl.ds(at, 8), :] = -LOG2E * jnp.exp(other_log[:, lanes])
            skips.append(skip[:, lanes])
    skip = jnp.concatenate(skips, 0)
    for n in range(16):
        rate_ref[0, 8 * n : 8 * n + 8, :] = par_scr[pl.ds(n, 8, stride=16), :]
    rates = [rate_ref[0, 8 * n : 8 * n + 8, :] for n in range(16)]

    def advance(t, carry):
        total, state = carry
        at = pl.multiple_of(t * 8, 8)
        now = step_ref[0, pl.ds(at, 8), :]
        xt = x_scr[pl.ds(at, 8), :]
        drive = now * xt
        even = skip * xt
        odd = None
        fresh = []
        for n in range(16):
            b = row_of(bc_ref, n * rows + t)
            c = row_of(bc_ref, (16 + n) * rows + t)
            h = jnp.exp2(now * rates[n]) * state[n] + b * drive
            fresh.append(h)
            if n % 2:
                odd = c * h if odd is None else odd + c * h
            else:
                even = even + c * h
        y_ref[0, pl.ds(at, 8), :] = even + odd
        return total + now, tuple(fresh)

    zero = jnp.zeros((8, 128), F32)
    total, state = lax.fori_loop(0, rows, advance, (zero, (zero,) * 16), unroll=8)
    for n in range(16):
        h_scr[8 * n : 8 * n + 8, :] = state[n]
    high = total.astype(BF16).astype(F32)
    h_scr[128:136, :] = high
    h_scr[136:144, :] = total - high
    for j in range(8):
        low = h_scr[pl.ds(j, 8, stride=8), :]
        up = h_scr[pl.ds(64 + j, 8, stride=8), :]
        ends_ref[j // 2, (j % 2) * 16 : (j % 2) * 16 + 16, :] = jnp.concatenate([low, up], 0).astype(BF16)
    for jj in range(4):
        sums = [h_scr[128 + 2 * jj : 130 + 2 * jj, :], h_scr[136 + 2 * jj : 138 + 2 * jj, :], jnp.zeros((4, 128), F32)]
        ends_ref[jj, 32:40, :] = jnp.concatenate(sums, 0).astype(BF16)


def scan(where, mine, other, gain, xc, d_own, d_oth):
    rows, inner = xc.shape
    blocks = inner // BLK
    wspec = pl.BlockSpec((1, 4, 152, 256), lambda b, where: (b // 2, b % 2, 0, 0))
    grid_spec = pltpu.PrefetchScalarGridSpec(
        num_scalar_prefetch=1,
        grid=(blocks,),
        in_specs=[
            pl.BlockSpec((rows, 288), lambda b, where: (0, 0)),
            pl.BlockSpec((rows, 288), lambda b, where: (0, 0)),
            pl.BlockSpec((1, 256), lambda b, where: (0, 0)),
            pl.BlockSpec((rows, BLK), lambda b, where: (0, b)),
            wspec,
            wspec,
        ],
        out_specs=[
            pl.BlockSpec((1, 8 * rows, 128), lambda b, where: (b, 0, 0)),
            pl.BlockSpec((1, 8 * rows, 128), lambda b, where: (b, 0, 0)),
            pl.BlockSpec((1, 128, 128), lambda b, where: (b, 0, 0)),
            pl.BlockSpec((4, 40, 128), lambda b, where: (b, 0, 0)),
        ],
        scratch_shapes=[
            pltpu.VMEM((8 * rows, 128), F32),
            pltpu.VMEM((128, 128), F32),
            pltpu.VMEM((144, 128), F32),
            pltpu.VMEM((rows, 256), BF16),
            pltpu.VMEM((32 * rows, 128), F32),
        ],
    )
    return pl.pallas_call(
        scan_kernel,
        grid_spec=grid_spec,
        out_shape=[
            jax.ShapeDtypeStruct((blocks, 8 * rows, 128), F32),
            jax.ShapeDtypeStruct((blocks, 8 * rows, 128), F32),
            jax.ShapeDtypeStruct((blocks, 128, 128), F32),
            jax.ShapeDtypeStruct((4 * blocks, 40, 128), BF16),
        ],
        compiler_params=pltpu.CompilerParams(dimension_semantics=("arbitrary",)),
        name="scan",
    )(where, mine, other, gain, xc, d_own, d_oth)


def link_kernel(ends_ref, log_ref, start_ref):
    count = ends_ref.shape[0]
    rate = -LOG2E * jnp.exp(log_ref[...])
    rate = jnp.concatenate([rate[:, 0:128], rate[:, 128:256]], 0)
    state = jnp.zeros((32, 128), F32)
    for s in range(count):
        start_ref[s] = state.astype(BF16)
        sums = ends_ref[s, 32:40, :].astype(F32)
        sums = sums[0:2] + sums[2:4]
        spread = jnp.concatenate([jnp.broadcast_to(sums[0:1], (16, 128)), jnp.broadcast_to(sums[1:2], (16, 128))], 0)
        state = jnp.exp2(rate * spread) * state + ends_ref[s, 0:32, :].astype(F32)


def link(ends, a_log):
    return pl.pallas_call(
        link_kernel,
        out_shape=jax.ShapeDtypeStruct((ends.shape[0], 32, 128), BF16),
        name="link",
    )(ends, a_log)


def close_kernel(step_ref, y_ref, rate_ref, start_ref, mine_ref, other_ref, gate_ref, out_ref, s_scr, y_scr, c_ref):
    rows = gate_ref.shape[0]

    @pl.when(pl.program_id(0) == 0)
    def _():
        spread(mine_ref[...] + other_ref[...], 272, 16, c_ref)

    for j in range(8):
        s_scr[16 * j : 16 * j + 16, :] = start_ref[j // 2, (j % 2) * 16 : (j % 2) * 16 + 16, :].astype(F32)
    starts = [s_scr[pl.ds(n, 8, stride=16), :] for n in range(16)]
    rates = [rate_ref[0, 8 * n : 8 * n + 8, :] for n in range(16)]

    def advance(t, total):
        at = pl.multiple_of(t * 8, 8)
        total = total + step_ref[0, pl.ds(at, 8), :]
        even = y_ref[0, pl.ds(at, 8), :]
        odd = None
        for n in range(16):
            c = row_of(c_ref, n * rows + t)
            part = c * starts[n] * jnp.exp2(total * rates[n])
            if n % 2:
                odd = part if odd is None else odd + part
            else:
                even = even + part
        y_scr[pl.ds(at, 8), :] = even + odd
        return total

    lax.fori_loop(0, rows, advance, jnp.zeros((8, 128), F32), unroll=8)
    for j in range(8):
        for i in range(rows // 16):
            low = y_scr[pl.ds(128 * i + j, 8, stride=8), :]
            up = y_scr[pl.ds(128 * i + 64 + j, 8, stride=8), :]
            y = jnp.concatenate([low, up], 0).astype(BF16).astype(F32)
            gate = gate_ref[16 * i : 16 * i + 16, j * 128 : (j + 1) * 128].astype(F32)
            out_ref[16 * i : 16 * i + 16, j * 128 : (j + 1) * 128] = (y * silu(gate)).astype(BF16)


def close(step, y, rate, start, mine, other, gate):
    rows, inner = gate.shape
    return pl.pallas_call(
        close_kernel,
        grid=(inner // BLK,),
        in_specs=[
            pl.BlockSpec((1, 8 * rows, 128), lambda b: (b, 0, 0)),
            pl.BlockSpec((1, 8 * rows, 128), lambda b: (b, 0, 0)),
            pl.BlockSpec((1, 128, 128), lambda b: (b, 0, 0)),
            pl.BlockSpec((4, 32, 128), lambda b: (b, 0, 0)),
            pl.BlockSpec((rows, 288), lambda b: (0, 0)),
            pl.BlockSpec((rows, 288), lambda b: (0, 0)),
            pl.BlockSpec((rows, BLK), lambda b: (0, b)),
        ],
        out_specs=pl.BlockSpec((rows, BLK), lambda b: (0, b)),
        out_shape=jax.ShapeDtypeStruct((rows, inner), BF16),
        scratch_shapes=[pltpu.VMEM((128, 128), F32), pltpu.VMEM((8 * rows, 128), F32), pltpu.VMEM((16 * rows, 128), F32)],
        compiler_params=pltpu.CompilerParams(dimension_semantics=("arbitrary",)),
        name="close",
    )(step, y, rate, start, mine, other, gate)


def from_everyone(x, axis):
    copies = jnp.broadcast_to(x, (lax.axis_size(axis), *x.shape))
    return lax.all_to_all(copies, axis, split_axis=0, concat_axis=0, tiled=True)


def pack_x(core, x_weight):
    return lax.dynamic_slice_in_dim(x_weight.T, core * 128, 128, 1)


def pack_d(core, dt_weight, dt_bias, a_log, skip, conv_weight, conv_bias):
    half = lax.dynamic_slice_in_dim(dt_weight, core * 128, 128, 0)
    logs = lax.dynamic_slice_in_dim(a_log, core * 8, 8, 0)
    vec = jnp.where(core == 0, dt_bias, skip)[None, :]
    pieces = [half, *two_parts(logs), *two_parts(vec), jnp.zeros((6, SHARD), BF16)]
    pieces += [conv_weight, conv_bias[None, :], jnp.zeros((3, SHARD), BF16)]
    return jnp.concatenate(pieces, 0)


def shifted(block, axis, by):
    count = lax.axis_size(axis)
    return lax.ppermute(block, axis, [(i, (i + by) % count) for i in range(count)])


def placed(blocks, at, axis):
    count = lax.axis_size(axis)
    here = lax.axis_index(axis)
    first = blocks[0]
    out = jnp.zeros((count, *first.shape), first.dtype)
    for block, (by, row) in zip(blocks, at):
        out = lax.dynamic_update_slice(out, block[None], ((here + by) % count, row) + (0,) * (first.ndim - 1))
    return out


def both_ways(pair, axis):
    return shifted(pair[0], axis, 1), shifted(pair[1], axis, -1)


def body(conv_input, gate_input, conv_weight, conv_bias, x_weight, dt_gain, dt_weight, dt_bias, a_log, skip):
    core = lax.axis_index("core")
    count = lax.axis_size(SEQ)
    swap = [(0, 1), (1, 0)]
    where = jnp.stack([core, lax.axis_index("z")]).astype(jnp.int32)
    x_piece = pack_x(core, x_weight)
    x_pieces = [x_piece] + [shifted(x_piece, "y", k) for k in (1, 2, 3)]
    x0 = placed(x_pieces, [(0, 0), (-1, 0), (-2, 0), (-3, 0)], "y")
    d_part = from_everyone(pack_d(core, dt_weight, dt_bias, a_log, skip, conv_weight, conv_bias), "z")
    d_part = d_part.reshape(8, 160, SHARD)
    prior = lax.ppermute(conv_input[conv_input.shape[0] - 8 :], SEQ, [(i, i + 1) for i in range(count - 1)])
    x1 = both_ways((x0, x0), "z")
    taps = from_everyone(d_part[:, 152:], "y").reshape(4, 8, 8, SHARD)
    x2 = both_ways(x1, "z")
    d0 = d_part[:, :152]
    up, down = both_ways((d0, d0), "y")
    xc, lend = conv(where, conv_input, prior, taps)
    x3 = both_ways(x2, "z")
    lent = lax.ppermute(lend, "core", swap)
    x4 = both_ways((x3[0][:2], x3[1][2:]), "z")
    d2 = both_ways((up[:4], down[4:]), "y")
    d_own = placed([d0, up, down, *d2], [(0, 0), (-1, 0), (1, 0), (2, 0), (2, 4)], "y")
    d_oth = lax.ppermute(d_own, "core", swap)
    mine, other = project(where, xc, lent, [x0, *x1, *x2, *x3, *x4])
    other = lax.ppermute(other, "core", swap)
    step, y, rate, ends = scan(where, mine, other, dt_gain[None, :], xc, d_own, d_oth)
    ends = lax.all_to_all(ends, SEQ, split_axis=0, concat_axis=0, tiled=True)
    start = lax.all_to_all(link(ends, a_log), SEQ, split_axis=0, concat_axis=0, tiled=True)
    return close(step, y, rate, start, mine, other, gate_input)


def solution(mesh):
    inner = Mesh(mesh.devices.reshape(4, 8, 4, 2), ("y", "z", "x", "core"))
    tokens = P(("x", "core", "y", "z"), None)
    return jax.shard_map(
        body,
        mesh=inner,
        in_specs=(tokens, tokens, P(None, SEQ), P(SEQ), P(SEQ, None), P(), P(None, SEQ), P(SEQ), P(None, SEQ), P(SEQ)),
        out_specs=tokens,
        check_vma=False,
    )
```

```python
import jax
import jax.numpy as jnp
from jax import lax
from jax.experimental import pallas as pl
from jax.experimental.pallas import tpu as pltpu
from jax.sharding import Mesh, PartitionSpec as P


F32 = jnp.float32
BF16 = jnp.bfloat16
LOG2E = 1.4426950408889634
SEQ = ("y", "z")
BLK = 1024
SHARD = 256


def silu(v):
    return v / (1.0 + jnp.exp(-v))


def row_of(ref, at):
    return ref[pl.ds(at, 8, stride=0), :]


def two_parts(v):
    high = lax.reduce_precision(v, 8, 7)
    return high.astype(BF16), (v - high).astype(BF16)


def conv_kernel(core_ref, ci_ref, prior_ref, par_ref, xc_ref, lend_ref, pad_ref):
    core = core_ref[0]
    rows = ci_ref.shape[0]
    taps = 4
    pad_ref[0:8, :] = prior_ref[...].astype(F32)
    pad_ref[8 : 8 + rows, :] = ci_ref[...].astype(F32)
    for s in range(4):
        par = par_ref[0, s].astype(F32)
        lanes = slice(s * SHARD, (s + 1) * SHARD)
        total = jnp.broadcast_to(par[taps : taps + 1, :], (rows, SHARD))
        for k in range(taps):
            total = total + par[k : k + 1, :] * pad_ref[5 + k : 5 + k + rows, lanes]
        xc_ref[:, lanes] = silu(total).astype(BF16)
        at = pl.multiple_of(s * SHARD + (1 - core) * 128, 128)
        lend_ref[:, s * 128 : (s + 1) * 128] = xc_ref[:, pl.ds(at, 128)]


def conv(core, conv_input, prior, params):
    rows, inner = conv_input.shape
    return pl.pallas_call(
        conv_kernel,
        grid=(inner // BLK,),
        in_specs=[
            pl.BlockSpec(memory_space=pltpu.SMEM),
            pl.BlockSpec((rows, BLK), lambda b: (0, b)),
            pl.BlockSpec((8, BLK), lambda b: (0, b)),
            pl.BlockSpec((1, 4, 8, SHARD), lambda b: (b // 2, b % 2, 0, 0)),
        ],
        out_specs=[
            pl.BlockSpec((rows, BLK), lambda b: (0, b)),
            pl.BlockSpec((rows, BLK // 2), lambda b: (0, b)),
        ],
        out_shape=[
            jax.ShapeDtypeStruct((rows, inner), BF16),
            jax.ShapeDtypeStruct((rows, inner // 2), BF16),
        ],
        scratch_shapes=[pltpu.VMEM((rows + 8, BLK), F32)],
        compiler_params=pltpu.CompilerParams(dimension_semantics=("arbitrary",)),
        name="conv",
    )(core, conv_input, prior, params)


def times_rows(left, right):
    return lax.dot_general(left, right, (((1,), (1,)), ((), ())), preferred_element_type=F32)


def project_kernel(where_ref, xc_ref, lent_ref, weight_ref, own_ref, other_ref):
    core = where_ref[0]
    rows = xc_ref.shape[0]
    depth, width = weight_ref.shape[:2]
    total = None
    for z in range(depth):
        for y in range(0, width, 2):
            left = []
            for shard in (y * depth + z, (y + 1) * depth + z):
                mine = pl.multiple_of(shard * SHARD + core * 128, 128)
                both = [xc_ref[:, pl.ds(mine, 128)], lent_ref[:, shard * 128 : (shard + 1) * 128]]
                left.append(jnp.concatenate(both, 0))
            right = jnp.concatenate([weight_ref[z, y], weight_ref[z, y + 1]], 1)
            part = times_rows(jnp.concatenate(left, 1), right)
            total = part if total is None else total + part
    own_ref[...] = total[:rows]
    other_ref[...] = total[rows:]


def project(where, xc, lent, weight):
    rows = xc.shape[0]
    vmem = pl.BlockSpec(memory_space=pltpu.VMEM)
    shape = jax.ShapeDtypeStruct((rows, 288), F32)
    return pl.pallas_call(
        project_kernel,
        in_specs=[pl.BlockSpec(memory_space=pltpu.SMEM), vmem, vmem, vmem],
        out_specs=[vmem, vmem],
        out_shape=[shape, shape],
        name="project",
    )(where, xc, lent, weight)


def spread(proj, first, count, out_ref):
    rows = proj.shape[0]
    for m in range(count):
        out_ref[m * rows : (m + 1) * rows, :] = jnp.broadcast_to(proj[:, first + m : first + m + 1], (rows, 128))


def scan_kernel(where_ref, mine_ref, other_ref, gain_ref, xc_ref, own_ref, oth_ref, step_ref, y_ref, rate_ref, ends_ref, *scratch):
    x_scr, par_scr, h_scr, normed_ref, bc_ref = scratch
    core = where_ref[0]
    rows = xc_ref.shape[0]
    rank = gain_ref.shape[1]

    @pl.when(pl.program_id(0) == 0)
    def _():
        proj = mine_ref[...] + other_ref[...]
        low = proj[:, 0:rank]
        scale = lax.rsqrt(jnp.mean(low * low, axis=1, keepdims=True) + 1e-06)
        normed_ref[...] = (low * scale * gain_ref[...]).astype(BF16)
        spread(proj, rank, 32, bc_ref)

    mine_k = normed_ref[:, pl.ds(pl.multiple_of(core * 128, 128), 128)]
    other_k = normed_ref[:, pl.ds(pl.multiple_of((1 - core) * 128, 128), 128)]
    skips = []
    for s in range(4):
        raw = jnp.dot(mine_k, own_ref[0, s, 0:128, :], preferred_element_type=F32)
        raw = raw + jnp.dot(other_k, oth_ref[0, s, 0:128, :], preferred_element_type=F32)
        mine = own_ref[0, s, 128:152, :].astype(F32)
        other = oth_ref[0, s, 128:152, :].astype(F32)
        mine_log = mine[0:8] + mine[8:16]
        other_log = other[0:8] + other[8:16]
        mine_vec = mine[16:17] + mine[17:18]
        other_vec = other[16:17] + other[17:18]
        bias = jnp.where(core == 0, mine_vec, other_vec)
        skip = jnp.where(core == 0, other_vec, mine_vec)
        raw = raw + bias
        step = jnp.maximum(raw, 0.0) + jnp.log1p(jnp.exp(-jnp.abs(raw)))
        xs = xc_ref[:, s * SHARD : (s + 1) * SHARD].astype(F32)
        for p in range(2):
            j = 2 * s + p
            lanes = slice(p * 128, (p + 1) * 128)
            for i in range(rows // 8):
                step_ref[0, pl.ds(64 * i + j, 8, stride=8), :] = step[8 * i : 8 * i + 8, lanes]
                x_scr[pl.ds(64 * i + j, 8, stride=8), :] = xs[8 * i : 8 * i + 8, lanes]
            at = pl.multiple_of(j * 16 + core * 8, 8)
            par_scr[pl.ds(at, 8), :] = -LOG2E * jnp.exp(mine_log[:, lanes])
            at = pl.multiple_of(j * 16 + (1 - core) * 8, 8)
            par_scr[pl.ds(at, 8), :] = -LOG2E * jnp.exp(other_log[:, lanes])
            skips.append(skip[:, lanes])
    skip = jnp.concatenate(skips, 0)
    for n in range(16):
        rate_ref[0, 8 * n : 8 * n + 8, :] = par_scr[pl.ds(n, 8, stride=16), :]
    rates = [rate_ref[0, 8 * n : 8 * n + 8, :] for n in range(16)]

    def advance(t, carry):
        total, state = carry
        at = pl.multiple_of(t * 8, 8)
        now = step_ref[0, pl.ds(at, 8), :]
        xt = x_scr[pl.ds(at, 8), :]
        drive = now * xt
        even = skip * xt
        odd = None
        fresh = []
        for n in range(16):
            b = row_of(bc_ref, n * rows + t)
            c = row_of(bc_ref, (16 + n) * rows + t)
            h = jnp.exp2(now * rates[n]) * state[n] + b * drive
            fresh.append(h)
            if n % 2:
                odd = c * h if odd is None else odd + c * h
            else:
                even = even + c * h
        y_ref[0, pl.ds(at, 8), :] = even + odd
        return total + now, tuple(fresh)

    zero = jnp.zeros((8, 128), F32)
    total, state = lax.fori_loop(0, rows, advance, (zero, (zero,) * 16), unroll=8)
    for n in range(16):
        h_scr[8 * n : 8 * n + 8, :] = state[n]
    high = total.astype(BF16).astype(F32)
    h_scr[128:136, :] = high
    h_scr[136:144, :] = total - high
    for j in range(8):
        low = h_scr[pl.ds(j, 8, stride=8), :]
        up = h_scr[pl.ds(64 + j, 8, stride=8), :]
        ends_ref[j // 2, (j % 2) * 16 : (j % 2) * 16 + 16, :] = jnp.concatenate([low, up], 0).astype(BF16)
    for jj in range(4):
        sums = [h_scr[128 + 2 * jj : 130 + 2 * jj, :], h_scr[136 + 2 * jj : 138 + 2 * jj, :], jnp.zeros((4, 128), F32)]
        ends_ref[jj, 32:40, :] = jnp.concatenate(sums, 0).astype(BF16)


def scan(where, mine, other, gain, xc, d_own, d_oth):
    rows, inner = xc.shape
    blocks = inner // BLK
    wspec = pl.BlockSpec((1, 4, 152, 256), lambda b, where: (b // 2, b % 2, 0, 0))
    grid_spec = pltpu.PrefetchScalarGridSpec(
        num_scalar_prefetch=1,
        grid=(blocks,),
        in_specs=[
            pl.BlockSpec((rows, 288), lambda b, where: (0, 0)),
            pl.BlockSpec((rows, 288), lambda b, where: (0, 0)),
            pl.BlockSpec((1, 256), lambda b, where: (0, 0)),
            pl.BlockSpec((rows, BLK), lambda b, where: (0, b)),
            wspec,
            wspec,
        ],
        out_specs=[
            pl.BlockSpec((1, 8 * rows, 128), lambda b, where: (b, 0, 0)),
            pl.BlockSpec((1, 8 * rows, 128), lambda b, where: (b, 0, 0)),
            pl.BlockSpec((1, 128, 128), lambda b, where: (b, 0, 0)),
            pl.BlockSpec((4, 40, 128), lambda b, where: (b, 0, 0)),
        ],
        scratch_shapes=[
            pltpu.VMEM((8 * rows, 128), F32),
            pltpu.VMEM((128, 128), F32),
            pltpu.VMEM((144, 128), F32),
            pltpu.VMEM((rows, 256), BF16),
            pltpu.VMEM((32 * rows, 128), F32),
        ],
    )
    return pl.pallas_call(
        scan_kernel,
        grid_spec=grid_spec,
        out_shape=[
            jax.ShapeDtypeStruct((blocks, 8 * rows, 128), F32),
            jax.ShapeDtypeStruct((blocks, 8 * rows, 128), F32),
            jax.ShapeDtypeStruct((blocks, 128, 128), F32),
            jax.ShapeDtypeStruct((4 * blocks, 40, 128), BF16),
        ],
        compiler_params=pltpu.CompilerParams(dimension_semantics=("arbitrary",)),
        name="scan",
    )(where, mine, other, gain, xc, d_own, d_oth)


def link_kernel(ends_ref, log_ref, start_ref):
    count = ends_ref.shape[0]
    rate = -LOG2E * jnp.exp(log_ref[...])
    rate = jnp.concatenate([rate[:, 0:128], rate[:, 128:256]], 0)
    state = jnp.zeros((32, 128), F32)
    for s in range(count):
        start_ref[s] = state.astype(BF16)
        sums = ends_ref[s, 32:40, :].astype(F32)
        sums = sums[0:2] + sums[2:4]
        spread = jnp.concatenate([jnp.broadcast_to(sums[0:1], (16, 128)), jnp.broadcast_to(sums[1:2], (16, 128))], 0)
        state = jnp.exp2(rate * spread) * state + ends_ref[s, 0:32, :].astype(F32)


def link(ends, a_log):
    return pl.pallas_call(
        link_kernel,
        out_shape=jax.ShapeDtypeStruct((ends.shape[0], 32, 128), BF16),
        name="link",
    )(ends, a_log)


def close_kernel(step_ref, y_ref, rate_ref, start_ref, mine_ref, other_ref, gate_ref, out_ref, s_scr, y_scr, c_ref):
    rows = gate_ref.shape[0]

    @pl.when(pl.program_id(0) == 0)
    def _():
        spread(mine_ref[...] + other_ref[...], 272, 16, c_ref)

    for j in range(8):
        s_scr[16 * j : 16 * j + 16, :] = start_ref[j // 2, (j % 2) * 16 : (j % 2) * 16 + 16, :].astype(F32)
    starts = [s_scr[pl.ds(n, 8, stride=16), :] for n in range(16)]
    rates = [rate_ref[0, 8 * n : 8 * n + 8, :] for n in range(16)]

    def advance(t, total):
        at = pl.multiple_of(t * 8, 8)
        total = total + step_ref[0, pl.ds(at, 8), :]
        even = y_ref[0, pl.ds(at, 8), :]
        odd = None
        for n in range(16):
            c = row_of(c_ref, n * rows + t)
            part = c * starts[n] * jnp.exp2(total * rates[n])
            if n % 2:
                odd = part if odd is None else odd + part
            else:
                even = even + part
        y_scr[pl.ds(at, 8), :] = even + odd
        return total

    lax.fori_loop(0, rows, advance, jnp.zeros((8, 128), F32), unroll=8)
    for j in range(8):
        for i in range(rows // 16):
            low = y_scr[pl.ds(128 * i + j, 8, stride=8), :]
            up = y_scr[pl.ds(128 * i + 64 + j, 8, stride=8), :]
            y = jnp.concatenate([low, up], 0).astype(BF16).astype(F32)
            gate = gate_ref[16 * i : 16 * i + 16, j * 128 : (j + 1) * 128].astype(F32)
            out_ref[16 * i : 16 * i + 16, j * 128 : (j + 1) * 128] = (y * silu(gate)).astype(BF16)


def close(step, y, rate, start, mine, other, gate):
    rows, inner = gate.shape
    return pl.pallas_call(
        close_kernel,
        grid=(inner // BLK,),
        in_specs=[
            pl.BlockSpec((1, 8 * rows, 128), lambda b: (b, 0, 0)),
            pl.BlockSpec((1, 8 * rows, 128), lambda b: (b, 0, 0)),
            pl.BlockSpec((1, 128, 128), lambda b: (b, 0, 0)),
            pl.BlockSpec((4, 32, 128), lambda b: (b, 0, 0)),
            pl.BlockSpec((rows, 288), lambda b: (0, 0)),
            pl.BlockSpec((rows, 288), lambda b: (0, 0)),
            pl.BlockSpec((rows, BLK), lambda b: (0, b)),
        ],
        out_specs=pl.BlockSpec((rows, BLK), lambda b: (0, b)),
        out_shape=jax.ShapeDtypeStruct((rows, inner), BF16),
        scratch_shapes=[pltpu.VMEM((128, 128), F32), pltpu.VMEM((8 * rows, 128), F32), pltpu.VMEM((16 * rows, 128), F32)],
        compiler_params=pltpu.CompilerParams(dimension_semantics=("arbitrary",)),
        name="close",
    )(step, y, rate, start, mine, other, gate)


def from_everyone(x, axis):
    copies = jnp.broadcast_to(x, (lax.axis_size(axis), *x.shape))
    return lax.all_to_all(copies, axis, split_axis=0, concat_axis=0, tiled=True)


def pack_x(core, x_weight):
    return lax.dynamic_slice_in_dim(x_weight.T, core * 128, 128, 1)


def pack_d(core, dt_weight, dt_bias, a_log, skip, conv_weight, conv_bias):
    half = lax.dynamic_slice_in_dim(dt_weight, core * 128, 128, 0)
    logs = lax.dynamic_slice_in_dim(a_log, core * 8, 8, 0)
    vec = jnp.where(core == 0, dt_bias, skip)[None, :]
    pieces = [half, *two_parts(logs), *two_parts(vec), jnp.zeros((6, SHARD), BF16)]
    pieces += [conv_weight, conv_bias[None, :], jnp.zeros((3, SHARD), BF16)]
    return jnp.concatenate(pieces, 0)


def shifted(block, axis, by):
    count = lax.axis_size(axis)
    return lax.ppermute(block, axis, [(i, (i + by) % count) for i in range(count)])


def placed(blocks, at, axis):
    count = lax.axis_size(axis)
    here = lax.axis_index(axis)
    first = blocks[0]
    out = jnp.zeros((count, *first.shape), first.dtype)
    for block, (by, row) in zip(blocks, at):
        out = lax.dynamic_update_slice(out, block[None], ((here + by) % count, row) + (0,) * (first.ndim - 1))
    return out


def both_ways(pair, axis):
    return shifted(pair[0], axis, 1), shifted(pair[1], axis, -1)


def body(conv_input, gate_input, conv_weight, conv_bias, x_weight, dt_gain, dt_weight, dt_bias, a_log, skip):
    core = lax.axis_index("core")
    count = lax.axis_size(SEQ)
    swap = [(0, 1), (1, 0)]
    where = jnp.stack([core, lax.axis_index("z")]).astype(jnp.int32)
    x_piece = pack_x(core, x_weight)
    x_pieces = [x_piece] + [shifted(x_piece, "y", k) for k in (1, 2, 3)]
    x0 = placed(x_pieces, [(0, 0), (-1, 0), (-2, 0), (-3, 0)], "y")
    d_part = from_everyone(pack_d(core, dt_weight, dt_bias, a_log, skip, conv_weight, conv_bias), "z")
    d_part = d_part.reshape(8, 160, SHARD)
    prior = lax.ppermute(conv_input[conv_input.shape[0] - 8 :], SEQ, [(i, i + 1) for i in range(count - 1)])
    x_own = lax.all_gather(x0, "z", axis=0)
    taps = from_everyone(d_part[:, 152:], "y").reshape(4, 8, 8, SHARD)
    d0 = d_part[:, :152]
    up, down = both_ways((d0, d0), "y")
    xc, lend = conv(where, conv_input, prior, taps)
    lent = lax.ppermute(lend, "core", swap)
    d2 = both_ways((up[:4], down[4:]), "y")
    d_own = placed([d0, up, down, *d2], [(0, 0), (-1, 0), (1, 0), (2, 0), (2, 4)], "y")
    d_oth = lax.ppermute(d_own, "core", swap)
    mine, other = project(where, xc, lent, x_own)
    other = lax.ppermute(other, "core", swap)
    step, y, rate, ends = scan(where, mine, other, dt_gain[None, :], xc, d_own, d_oth)
    ends = lax.all_to_all(ends, SEQ, split_axis=0, concat_axis=0, tiled=True)
    start = lax.all_to_all(link(ends, a_log), SEQ, split_axis=0, concat_axis=0, tiled=True)
    return close(step, y, rate, start, mine, other, gate_input)


def solution(mesh):
    inner = Mesh(mesh.devices.reshape(4, 8, 4, 2), ("y", "z", "x", "core"))
    tokens = P(("x", "core", "y", "z"), None)
    return jax.shard_map(
        body,
        mesh=inner,
        in_specs=(tokens, tokens, P(None, SEQ), P(SEQ), P(SEQ, None), P(), P(None, SEQ), P(SEQ), P(None, SEQ), P(SEQ)),
        out_specs=tokens,
        check_vma=False,
    )
```

```python
import jax
import jax.numpy as jnp
from jax import lax
from jax.experimental import pallas as pl
from jax.experimental.pallas import tpu as pltpu
from jax.sharding import Mesh, PartitionSpec as P


F32 = jnp.float32
BF16 = jnp.bfloat16
LOG2E = 1.4426950408889634
SEQ = ("y", "z")
BLK = 1024
SHARD = 256


def silu(v):
    return v / (1.0 + jnp.exp(-v))


def row_of(ref, at):
    return ref[pl.ds(at, 8, stride=0), :]


def two_parts(v):
    high = lax.reduce_precision(v, 8, 7)
    return high.astype(BF16), (v - high).astype(BF16)


def conv_kernel(core_ref, ci_ref, prior_ref, par_ref, xc_ref, lend_ref, pad_ref):
    core = core_ref[0]
    rows = ci_ref.shape[0]
    taps = 4
    pad_ref[0:8, :] = prior_ref[...].astype(F32)
    pad_ref[8 : 8 + rows, :] = ci_ref[...].astype(F32)
    for s in range(4):
        par = par_ref[0, s].astype(F32)
        lanes = slice(s * SHARD, (s + 1) * SHARD)
        total = jnp.broadcast_to(par[taps : taps + 1, :], (rows, SHARD))
        for k in range(taps):
            total = total + par[k : k + 1, :] * pad_ref[5 + k : 5 + k + rows, lanes]
        xc_ref[:, lanes] = silu(total).astype(BF16)
        at = pl.multiple_of(s * SHARD + (1 - core) * 128, 128)
        lend_ref[:, s * 128 : (s + 1) * 128] = xc_ref[:, pl.ds(at, 128)]


def conv(core, conv_input, prior, params):
    rows, inner = conv_input.shape
    return pl.pallas_call(
        conv_kernel,
        grid=(inner // BLK,),
        in_specs=[
            pl.BlockSpec(memory_space=pltpu.SMEM),
            pl.BlockSpec((rows, BLK), lambda b: (0, b)),
            pl.BlockSpec((8, BLK), lambda b: (0, b)),
            pl.BlockSpec((1, 4, 8, SHARD), lambda b: (b // 2, b % 2, 0, 0)),
        ],
        out_specs=[
            pl.BlockSpec((rows, BLK), lambda b: (0, b)),
            pl.BlockSpec((rows, BLK // 2), lambda b: (0, b)),
        ],
        out_shape=[
            jax.ShapeDtypeStruct((rows, inner), BF16),
            jax.ShapeDtypeStruct((rows, inner // 2), BF16),
        ],
        scratch_shapes=[pltpu.VMEM((rows + 8, BLK), F32)],
        compiler_params=pltpu.CompilerParams(dimension_semantics=("arbitrary",)),
        name="conv",
    )(core, conv_input, prior, params)


AWAY = (0, -1, 1, -2, 2, -3, 3, 4)


def times_rows(left, right):
    return lax.dot_general(left, right, (((1,), (1,)), ((), ())), preferred_element_type=F32)


def project_kernel(where_ref, xc_ref, lent_ref, *refs):
    blocks, (own_ref, other_ref) = refs[:-2], refs[-2:]
    core, here = where_ref[0], where_ref[1]
    rows = xc_ref.shape[0]
    total = None
    for away, block in zip(AWAY, blocks):
        z = lax.rem(here + 8 + away, 8)
        for row in range(0, block.shape[0], 2):
            left = []
            for y in (row, row + 1):
                mine = pl.multiple_of((y * 8 + z) * SHARD + core * 128, 128)
                lent = pl.multiple_of((y * 8 + z) * 128, 128)
                left.append(jnp.concatenate([xc_ref[:, pl.ds(mine, 128)], lent_ref[:, pl.ds(lent, 128)]], 0))
            right = jnp.concatenate([block[row, 0:288, :], block[row + 1, 0:288, :]], 1)
            part = times_rows(jnp.concatenate(left, 1), right)
            total = part if total is None else total + part
    own_ref[...] = total[:rows]
    other_ref[...] = total[rows:]


def project(where, xc, lent, blocks):
    rows = xc.shape[0]
    vmem = pl.BlockSpec(memory_space=pltpu.VMEM)
    shape = jax.ShapeDtypeStruct((rows, 288), F32)
    return pl.pallas_call(
        project_kernel,
        in_specs=[pl.BlockSpec(memory_space=pltpu.SMEM)] + [vmem] * (2 + len(blocks)),
        out_specs=[vmem, vmem],
        out_shape=[shape, shape],
        name="project",
    )(where, xc, lent, *blocks)


def spread(proj, first, count, out_ref):
    rows = proj.shape[0]
    for m in range(count):
        out_ref[m * rows : (m + 1) * rows, :] = jnp.broadcast_to(proj[:, first + m : first + m + 1], (rows, 128))


def scan_kernel(where_ref, mine_ref, other_ref, gain_ref, xc_ref, own_ref, oth_ref, step_ref, y_ref, rate_ref, ends_ref, *scratch):
    x_scr, par_scr, h_scr, normed_ref, bc_ref = scratch
    core = where_ref[0]
    rows = xc_ref.shape[0]
    rank = gain_ref.shape[1]

    @pl.when(pl.program_id(0) == 0)
    def _():
        proj = mine_ref[...] + other_ref[...]
        low = proj[:, 0:rank]
        scale = lax.rsqrt(jnp.mean(low * low, axis=1, keepdims=True) + 1e-06)
        normed_ref[...] = (low * scale * gain_ref[...]).astype(BF16)
        spread(proj, rank, 32, bc_ref)

    mine_k = normed_ref[:, pl.ds(pl.multiple_of(core * 128, 128), 128)]
    other_k = normed_ref[:, pl.ds(pl.multiple_of((1 - core) * 128, 128), 128)]
    skips = []
    for s in range(4):
        raw = jnp.dot(mine_k, own_ref[0, s, 0:128, :], preferred_element_type=F32)
        raw = raw + jnp.dot(other_k, oth_ref[0, s, 0:128, :], preferred_element_type=F32)
        mine = own_ref[0, s, 128:152, :].astype(F32)
        other = oth_ref[0, s, 128:152, :].astype(F32)
        mine_log = mine[0:8] + mine[8:16]
        other_log = other[0:8] + other[8:16]
        mine_vec = mine[16:17] + mine[17:18]
        other_vec = other[16:17] + other[17:18]
        bias = jnp.where(core == 0, mine_vec, other_vec)
        skip = jnp.where(core == 0, other_vec, mine_vec)
        raw = raw + bias
        step = jnp.maximum(raw, 0.0) + jnp.log1p(jnp.exp(-jnp.abs(raw)))
        xs = xc_ref[:, s * SHARD : (s + 1) * SHARD].astype(F32)
        for p in range(2):
            j = 2 * s + p
            lanes = slice(p * 128, (p + 1) * 128)
            for i in range(rows // 8):
                step_ref[0, pl.ds(64 * i + j, 8, stride=8), :] = step[8 * i : 8 * i + 8, lanes]
                x_scr[pl.ds(64 * i + j, 8, stride=8), :] = xs[8 * i : 8 * i + 8, lanes]
            at = pl.multiple_of(j * 16 + core * 8, 8)
            par_scr[pl.ds(at, 8), :] = -LOG2E * jnp.exp(mine_log[:, lanes])
            at = pl.multiple_of(j * 16 + (1 - core) * 8, 8)
            par_scr[pl.ds(at, 8), :] = -LOG2E * jnp.exp(other_log[:, lanes])
            skips.append(skip[:, lanes])
    skip = jnp.concatenate(skips, 0)
    for n in range(16):
        rate_ref[0, 8 * n : 8 * n + 8, :] = par_scr[pl.ds(n, 8, stride=16), :]
    rates = [rate_ref[0, 8 * n : 8 * n + 8, :] for n in range(16)]

    def advance(t, carry):
        total, state = carry
        at = pl.multiple_of(t * 8, 8)
        now = step_ref[0, pl.ds(at, 8), :]
        xt = x_scr[pl.ds(at, 8), :]
        drive = now * xt
        even = skip * xt
        odd = None
        fresh = []
        for n in range(16):
            b = row_of(bc_ref, n * rows + t)
            c = row_of(bc_ref, (16 + n) * rows + t)
            h = jnp.exp2(now * rates[n]) * state[n] + b * drive
            fresh.append(h)
            if n % 2:
                odd = c * h if odd is None else odd + c * h
            else:
                even = even + c * h
        y_ref[0, pl.ds(at, 8), :] = even + odd
        return total + now, tuple(fresh)

    zero = jnp.zeros((8, 128), F32)
    total, state = lax.fori_loop(0, rows, advance, (zero, (zero,) * 16), unroll=8)
    for n in range(16):
        h_scr[8 * n : 8 * n + 8, :] = state[n]
    high = total.astype(BF16).astype(F32)
    h_scr[128:136, :] = high
    h_scr[136:144, :] = total - high
    for j in range(8):
        low = h_scr[pl.ds(j, 8, stride=8), :]
        up = h_scr[pl.ds(64 + j, 8, stride=8), :]
        ends_ref[j // 2, (j % 2) * 16 : (j % 2) * 16 + 16, :] = jnp.concatenate([low, up], 0).astype(BF16)
    for jj in range(4):
        sums = [h_scr[128 + 2 * jj : 130 + 2 * jj, :], h_scr[136 + 2 * jj : 138 + 2 * jj, :], jnp.zeros((4, 128), F32)]
        ends_ref[jj, 32:40, :] = jnp.concatenate(sums, 0).astype(BF16)


def scan(where, mine, other, gain, xc, d_own, d_oth):
    rows, inner = xc.shape
    blocks = inner // BLK
    wspec = pl.BlockSpec((1, 4, 152, 256), lambda b, where: (b // 2, b % 2, 0, 0))
    grid_spec = pltpu.PrefetchScalarGridSpec(
        num_scalar_prefetch=1,
        grid=(blocks,),
        in_specs=[
            pl.BlockSpec((rows, 288), lambda b, where: (0, 0)),
            pl.BlockSpec((rows, 288), lambda b, where: (0, 0)),
            pl.BlockSpec((1, 256), lambda b, where: (0, 0)),
            pl.BlockSpec((rows, BLK), lambda b, where: (0, b)),
            wspec,
            wspec,
        ],
        out_specs=[
            pl.BlockSpec((1, 8 * rows, 128), lambda b, where: (b, 0, 0)),
            pl.BlockSpec((1, 8 * rows, 128), lambda b, where: (b, 0, 0)),
            pl.BlockSpec((1, 128, 128), lambda b, where: (b, 0, 0)),
            pl.BlockSpec((4, 40, 128), lambda b, where: (b, 0, 0)),
        ],
        scratch_shapes=[
            pltpu.VMEM((8 * rows, 128), F32),
            pltpu.VMEM((128, 128), F32),
            pltpu.VMEM((144, 128), F32),
            pltpu.VMEM((rows, 256), BF16),
            pltpu.VMEM((32 * rows, 128), F32),
        ],
    )
    return pl.pallas_call(
        scan_kernel,
        grid_spec=grid_spec,
        out_shape=[
            jax.ShapeDtypeStruct((blocks, 8 * rows, 128), F32),
            jax.ShapeDtypeStruct((blocks, 8 * rows, 128), F32),
            jax.ShapeDtypeStruct((blocks, 128, 128), F32),
            jax.ShapeDtypeStruct((4 * blocks, 40, 128), BF16),
        ],
        compiler_params=pltpu.CompilerParams(dimension_semantics=("arbitrary",)),
        name="scan",
    )(where, mine, other, gain, xc, d_own, d_oth)


def link_kernel(ends_ref, log_ref, start_ref):
    count = ends_ref.shape[0]
    rate = -LOG2E * jnp.exp(log_ref[...])
    rate = jnp.concatenate([rate[:, 0:128], rate[:, 128:256]], 0)
    state = jnp.zeros((32, 128), F32)
    for s in range(count):
        start_ref[s] = state.astype(BF16)
        sums = ends_ref[s, 32:40, :].astype(F32)
        sums = sums[0:2] + sums[2:4]
        spread = jnp.concatenate([jnp.broadcast_to(sums[0:1], (16, 128)), jnp.broadcast_to(sums[1:2], (16, 128))], 0)
        state = jnp.exp2(rate * spread) * state + ends_ref[s, 0:32, :].astype(F32)


def link(ends, a_log):
    return pl.pallas_call(
        link_kernel,
        out_shape=jax.ShapeDtypeStruct((ends.shape[0], 32, 128), BF16),
        name="link",
    )(ends, a_log)


def close_kernel(step_ref, y_ref, rate_ref, start_ref, mine_ref, other_ref, gate_ref, out_ref, s_scr, y_scr, c_ref):
    rows = gate_ref.shape[0]

    @pl.when(pl.program_id(0) == 0)
    def _():
        spread(mine_ref[...] + other_ref[...], 272, 16, c_ref)

    for j in range(8):
        s_scr[16 * j : 16 * j + 16, :] = start_ref[j // 2, (j % 2) * 16 : (j % 2) * 16 + 16, :].astype(F32)
    starts = [s_scr[pl.ds(n, 8, stride=16), :] for n in range(16)]
    rates = [rate_ref[0, 8 * n : 8 * n + 8, :] for n in range(16)]

    def advance(t, total):
        at = pl.multiple_of(t * 8, 8)
        total = total + step_ref[0, pl.ds(at, 8), :]
        even = y_ref[0, pl.ds(at, 8), :]
        odd = None
        for n in range(16):
            c = row_of(c_ref, n * rows + t)
            part = c * starts[n] * jnp.exp2(total * rates[n])
            if n % 2:
                odd = part if odd is None else odd + part
            else:
                even = even + part
        y_scr[pl.ds(at, 8), :] = even + odd
        return total

    lax.fori_loop(0, rows, advance, jnp.zeros((8, 128), F32), unroll=8)
    for j in range(8):
        for i in range(rows // 16):
            low = y_scr[pl.ds(128 * i + j, 8, stride=8), :]
            up = y_scr[pl.ds(128 * i + 64 + j, 8, stride=8), :]
            y = jnp.concatenate([low, up], 0).astype(BF16).astype(F32)
            gate = gate_ref[16 * i : 16 * i + 16, j * 128 : (j + 1) * 128].astype(F32)
            out_ref[16 * i : 16 * i + 16, j * 128 : (j + 1) * 128] = (y * silu(gate)).astype(BF16)


def close(step, y, rate, start, mine, other, gate):
    rows, inner = gate.shape
    return pl.pallas_call(
        close_kernel,
        grid=(inner // BLK,),
        in_specs=[
            pl.BlockSpec((1, 8 * rows, 128), lambda b: (b, 0, 0)),
            pl.BlockSpec((1, 8 * rows, 128), lambda b: (b, 0, 0)),
            pl.BlockSpec((1, 128, 128), lambda b: (b, 0, 0)),
            pl.BlockSpec((4, 32, 128), lambda b: (b, 0, 0)),
            pl.BlockSpec((rows, 288), lambda b: (0, 0)),
            pl.BlockSpec((rows, 288), lambda b: (0, 0)),
            pl.BlockSpec((rows, BLK), lambda b: (0, b)),
        ],
        out_specs=pl.BlockSpec((rows, BLK), lambda b: (0, b)),
        out_shape=jax.ShapeDtypeStruct((rows, inner), BF16),
        scratch_shapes=[pltpu.VMEM((128, 128), F32), pltpu.VMEM((8 * rows, 128), F32), pltpu.VMEM((16 * rows, 128), F32)],
        compiler_params=pltpu.CompilerParams(dimension_semantics=("arbitrary",)),
        name="close",
    )(step, y, rate, start, mine, other, gate)


def from_everyone(x, axis):
    copies = jnp.broadcast_to(x, (lax.axis_size(axis), *x.shape))
    return lax.all_to_all(copies, axis, split_axis=0, concat_axis=0, tiled=True)


def pack_x(core, x_weight):
    return lax.dynamic_slice_in_dim(x_weight.T, core * 128, 128, 1)


def pack_d(core, dt_weight, dt_bias, a_log, skip, conv_weight, conv_bias):
    half = lax.dynamic_slice_in_dim(dt_weight, core * 128, 128, 0)
    logs = lax.dynamic_slice_in_dim(a_log, core * 8, 8, 0)
    vec = jnp.where(core == 0, dt_bias, skip)[None, :]
    pieces = [half, *two_parts(logs), *two_parts(vec), jnp.zeros((6, SHARD), BF16)]
    pieces += [conv_weight, conv_bias[None, :], jnp.zeros((3, SHARD), BF16)]
    return jnp.concatenate(pieces, 0)


def shifted(block, axis, by):
    count = lax.axis_size(axis)
    return lax.ppermute(block, axis, [(i, (i + by) % count) for i in range(count)])


def placed(blocks, at, axis):
    count = lax.axis_size(axis)
    here = lax.axis_index(axis)
    first = blocks[0]
    out = jnp.zeros((count, *first.shape), first.dtype)
    for block, (by, row) in zip(blocks, at):
        out = lax.dynamic_update_slice(out, block[None], ((here + by) % count, row) + (0,) * (first.ndim - 1))
    return out


def from_opposite(core, up, down, axis):
    count = lax.axis_size(axis)
    pairs = [(2 * i + c, 2 * ((i + 1 - 2 * c) % count) + c) for i in range(count) for c in range(2)]
    return lax.ppermute(jnp.where(core == 0, up, down), (axis, "core"), pairs)


def both_ways(pair, axis):
    return shifted(pair[0], axis, 1), shifted(pair[1], axis, -1)


def body(conv_input, gate_input, conv_weight, conv_bias, x_weight, dt_gain, dt_weight, dt_bias, a_log, skip):
    core = lax.axis_index("core")
    count = lax.axis_size(SEQ)
    swap = [(0, 1), (1, 0)]
    where = jnp.stack([core, lax.axis_index("z")]).astype(jnp.int32)
    x_piece = pack_x(core, x_weight)
    x_pieces = [x_piece] + [shifted(x_piece, "y", k) for k in (1, 2, 3)]
    x0 = placed(x_pieces, [(0, 0), (-1, 0), (-2, 0), (-3, 0)], "y")
    d_part = from_everyone(pack_d(core, dt_weight, dt_bias, a_log, skip, conv_weight, conv_bias), "z")
    d_part = d_part.reshape(8, 160, SHARD)
    prior = lax.ppermute(conv_input[conv_input.shape[0] - 8 :], SEQ, [(i, i + 1) for i in range(count - 1)])
    x1 = both_ways((x0, x0), "z")
    taps = from_everyone(d_part[:, 152:], "y").reshape(4, 8, 8, SHARD)
    x2 = both_ways(x1, "z")
    d0 = d_part[:, :152]
    up, down = both_ways((d0, d0), "y")
    xc, lend = conv(where, conv_input, prior, taps)
    x3 = both_ways(x2, "z")
    lent = lax.ppermute(lend, "core", swap)
    x4 = from_opposite(core, *x3, "z")
    d2 = from_opposite(core, up, down, "y")
    d_own = placed([d0, up, down, d2], [(0, 0), (-1, 0), (1, 0), (2, 0)], "y")
    d_oth = lax.ppermute(d_own, "core", swap)
    mine, other = project(where, xc, lent, [x0, *x1, *x2, *x3, x4])
    other = lax.ppermute(other, "core", swap)
    step, y, rate, ends = scan(where, mine, other, dt_gain[None, :], xc, d_own, d_oth)
    ends = lax.all_to_all(ends, SEQ, split_axis=0, concat_axis=0, tiled=True)
    start = lax.all_to_all(link(ends, a_log), SEQ, split_axis=0, concat_axis=0, tiled=True)
    return close(step, y, rate, start, mine, other, gate_input)


def solution(mesh):
    inner = Mesh(mesh.devices.reshape(4, 8, 4, 2), ("y", "z", "x", "core"))
    tokens = P(("x", "core", "y", "z"), None)
    return jax.shard_map(
        body,
        mesh=inner,
        in_specs=(tokens, tokens, P(None, SEQ), P(SEQ), P(SEQ, None), P(), P(None, SEQ), P(SEQ), P(None, SEQ), P(SEQ)),
        out_specs=tokens,
        check_vma=False,
    )
```

```python
import jax
import jax.numpy as jnp
from jax import lax
from jax.experimental import pallas as pl
from jax.experimental.pallas import tpu as pltpu
from jax.sharding import Mesh, PartitionSpec as P


F32 = jnp.float32
BF16 = jnp.bfloat16
LOG2E = 1.4426950408889634
SEQ = ("y", "z")
BLK = 1024
SHARD = 256


def silu(v):
    return v / (1.0 + jnp.exp(-v))


def row_of(ref, at):
    return ref[pl.ds(at, 8, stride=0), :]


def two_parts(v):
    high = lax.reduce_precision(v, 8, 7)
    return high.astype(BF16), (v - high).astype(BF16)


def conv_kernel(core_ref, ci_ref, prior_ref, par_ref, xc_ref, lend_ref, pad_ref):
    core = core_ref[0]
    rows = ci_ref.shape[0]
    taps = 4
    pad_ref[0:8, :] = prior_ref[...].astype(F32)
    pad_ref[8 : 8 + rows, :] = ci_ref[...].astype(F32)
    for s in range(4):
        par = par_ref[0, s].astype(F32)
        lanes = slice(s * SHARD, (s + 1) * SHARD)
        total = jnp.broadcast_to(par[taps : taps + 1, :], (rows, SHARD))
        for k in range(taps):
            total = total + par[k : k + 1, :] * pad_ref[5 + k : 5 + k + rows, lanes]
        xc_ref[:, lanes] = silu(total).astype(BF16)
        at = pl.multiple_of(s * SHARD + (1 - core) * 128, 128)
        lend_ref[:, s * 128 : (s + 1) * 128] = xc_ref[:, pl.ds(at, 128)]


def conv(core, conv_input, prior, params):
    rows, inner = conv_input.shape
    return pl.pallas_call(
        conv_kernel,
        grid=(inner // BLK,),
        in_specs=[
            pl.BlockSpec(memory_space=pltpu.SMEM),
            pl.BlockSpec((rows, BLK), lambda b: (0, b)),
            pl.BlockSpec((8, BLK), lambda b: (0, b)),
            pl.BlockSpec((1, 4, 8, SHARD), lambda b: (b // 2, b % 2, 0, 0)),
        ],
        out_specs=[
            pl.BlockSpec((rows, BLK), lambda b: (0, b)),
            pl.BlockSpec((rows, BLK // 2), lambda b: (0, b)),
        ],
        out_shape=[
            jax.ShapeDtypeStruct((rows, inner), BF16),
            jax.ShapeDtypeStruct((rows, inner // 2), BF16),
        ],
        scratch_shapes=[pltpu.VMEM((rows + 8, BLK), F32)],
        compiler_params=pltpu.CompilerParams(dimension_semantics=("arbitrary",)),
        name="conv",
    )(core, conv_input, prior, params)


AWAY = (0, -1, 1, -2, 2, -3, 3, 4)


def times_rows(left, right):
    return lax.dot_general(left, right, (((1,), (1,)), ((), ())), preferred_element_type=F32)


def project_kernel(where_ref, xc_ref, lent_ref, *refs):
    blocks, (own_ref, other_ref) = refs[:-2], refs[-2:]
    core, here = where_ref[0], where_ref[1]
    rows = xc_ref.shape[0]
    total = None
    for away, block in zip(AWAY, blocks):
        z = lax.rem(here + 8 + away, 8)
        for row in range(0, block.shape[0], 2):
            left = []
            for y in (row, row + 1):
                mine = pl.multiple_of((y * 8 + z) * SHARD + core * 128, 128)
                lent = pl.multiple_of((y * 8 + z) * 128, 128)
                left.append(jnp.concatenate([xc_ref[:, pl.ds(mine, 128)], lent_ref[:, pl.ds(lent, 128)]], 0))
            right = jnp.concatenate([block[row, 0:288, :], block[row + 1, 0:288, :]], 1)
            part = times_rows(jnp.concatenate(left, 1), right)
            total = part if total is None else total + part
    own_ref[...] = total[:rows]
    other_ref[...] = total[rows:]


def project(where, xc, lent, blocks):
    rows = xc.shape[0]
    vmem = pl.BlockSpec(memory_space=pltpu.VMEM)
    shape = jax.ShapeDtypeStruct((rows, 288), F32)
    return pl.pallas_call(
        project_kernel,
        in_specs=[pl.BlockSpec(memory_space=pltpu.SMEM)] + [vmem] * (2 + len(blocks)),
        out_specs=[vmem, vmem],
        out_shape=[shape, shape],
        name="project",
    )(where, xc, lent, *blocks)


def spread(proj, first, count, out_ref):
    rows = proj.shape[0]
    for m in range(count):
        out_ref[m * rows : (m + 1) * rows, :] = jnp.broadcast_to(proj[:, first + m : first + m + 1], (rows, 128))


def joined(ref, s):
    return jnp.concatenate([ref[0, q, s, 0:32, :] for q in range(4)], 0)


def extras(ref, s):
    parts = [ref[0, q, s, 32:40, :].astype(F32) for q in range(4)]
    return jnp.concatenate([p[0:2] + p[2:4] for p in parts], 0), parts[0][4:5] + parts[0][5:6]


def scan_kernel(where_ref, mine_ref, other_ref, gain_ref, xc_ref, own_ref, oth_ref, step_ref, y_ref, rate_ref, ends_ref, *scratch):
    x_scr, par_scr, h_scr, normed_ref, bc_ref = scratch
    core = where_ref[0]
    rows = xc_ref.shape[0]
    rank = gain_ref.shape[1]

    @pl.when(pl.program_id(0) == 0)
    def _():
        proj = mine_ref[...] + other_ref[...]
        low = proj[:, 0:rank]
        scale = lax.rsqrt(jnp.mean(low * low, axis=1, keepdims=True) + 1e-06)
        normed_ref[...] = (low * scale * gain_ref[...]).astype(BF16)
        spread(proj, rank, 32, bc_ref)

    mine_k = normed_ref[:, pl.ds(pl.multiple_of(core * 128, 128), 128)]
    other_k = normed_ref[:, pl.ds(pl.multiple_of((1 - core) * 128, 128), 128)]
    skips = []
    for s in range(4):
        raw = jnp.dot(mine_k, joined(own_ref, s), preferred_element_type=F32)
        raw = raw + jnp.dot(other_k, joined(oth_ref, s), preferred_element_type=F32)
        mine_log, mine_vec = extras(own_ref, s)
        other_log, other_vec = extras(oth_ref, s)
        bias = jnp.where(core == 0, mine_vec, other_vec)
        skip = jnp.where(core == 0, other_vec, mine_vec)
        raw = raw + bias
        step = jnp.maximum(raw, 0.0) + jnp.log1p(jnp.exp(-jnp.abs(raw)))
        xs = xc_ref[:, s * SHARD : (s + 1) * SHARD].astype(F32)
        for p in range(2):
            j = 2 * s + p
            lanes = slice(p * 128, (p + 1) * 128)
            for i in range(rows // 8):
                step_ref[0, pl.ds(64 * i + j, 8, stride=8), :] = step[8 * i : 8 * i + 8, lanes]
                x_scr[pl.ds(64 * i + j, 8, stride=8), :] = xs[8 * i : 8 * i + 8, lanes]
            at = pl.multiple_of(j * 16 + core * 8, 8)
            par_scr[pl.ds(at, 8), :] = -LOG2E * jnp.exp(mine_log[:, lanes])
            at = pl.multiple_of(j * 16 + (1 - core) * 8, 8)
            par_scr[pl.ds(at, 8), :] = -LOG2E * jnp.exp(other_log[:, lanes])
            skips.append(skip[:, lanes])
    skip = jnp.concatenate(skips, 0)
    for n in range(16):
        rate_ref[0, 8 * n : 8 * n + 8, :] = par_scr[pl.ds(n, 8, stride=16), :]
    rates = [rate_ref[0, 8 * n : 8 * n + 8, :] for n in range(16)]

    def advance(t, carry):
        total, state = carry
        at = pl.multiple_of(t * 8, 8)
        now = step_ref[0, pl.ds(at, 8), :]
        xt = x_scr[pl.ds(at, 8), :]
        drive = now * xt
        even = skip * xt
        odd = None
        fresh = []
        for n in range(16):
            b = row_of(bc_ref, n * rows + t)
            c = row_of(bc_ref, (16 + n) * rows + t)
            h = jnp.exp2(now * rates[n]) * state[n] + b * drive
            fresh.append(h)
            if n % 2:
                odd = c * h if odd is None else odd + c * h
            else:
                even = even + c * h
        y_ref[0, pl.ds(at, 8), :] = even + odd
        return total + now, tuple(fresh)

    zero = jnp.zeros((8, 128), F32)
    total, state = lax.fori_loop(0, rows, advance, (zero, (zero,) * 16), unroll=8)
    for n in range(16):
        h_scr[8 * n : 8 * n + 8, :] = state[n]
    high = total.astype(BF16).astype(F32)
    h_scr[128:136, :] = high
    h_scr[136:144, :] = total - high
    for j in range(8):
        low = h_scr[pl.ds(j, 8, stride=8), :]
        up = h_scr[pl.ds(64 + j, 8, stride=8), :]
        ends_ref[j // 2, (j % 2) * 16 : (j % 2) * 16 + 16, :] = jnp.concatenate([low, up], 0).astype(BF16)
    for jj in range(4):
        sums = [h_scr[128 + 2 * jj : 130 + 2 * jj, :], h_scr[136 + 2 * jj : 138 + 2 * jj, :], jnp.zeros((4, 128), F32)]
        ends_ref[jj, 32:40, :] = jnp.concatenate(sums, 0).astype(BF16)


def scan(where, mine, other, gain, xc, d_own, d_oth):
    rows, inner = xc.shape
    blocks = inner // BLK
    wspec = pl.BlockSpec((1, 4, 4, 40, 256), lambda b, where: (b // 2, 0, b % 2, 0, 0))
    grid_spec = pltpu.PrefetchScalarGridSpec(
        num_scalar_prefetch=1,
        grid=(blocks,),
        in_specs=[
            pl.BlockSpec((rows, 288), lambda b, where: (0, 0)),
            pl.BlockSpec((rows, 288), lambda b, where: (0, 0)),
            pl.BlockSpec((1, 256), lambda b, where: (0, 0)),
            pl.BlockSpec((rows, BLK), lambda b, where: (0, b)),
            wspec,
            wspec,
        ],
        out_specs=[
            pl.BlockSpec((1, 8 * rows, 128), lambda b, where: (b, 0, 0)),
            pl.BlockSpec((1, 8 * rows, 128), lambda b, where: (b, 0, 0)),
            pl.BlockSpec((1, 128, 128), lambda b, where: (b, 0, 0)),
            pl.BlockSpec((4, 40, 128), lambda b, where: (b, 0, 0)),
        ],
        scratch_shapes=[
            pltpu.VMEM((8 * rows, 128), F32),
            pltpu.VMEM((128, 128), F32),
            pltpu.VMEM((144, 128), F32),
            pltpu.VMEM((rows, 256), BF16),
            pltpu.VMEM((32 * rows, 128), F32),
        ],
    )
    return pl.pallas_call(
        scan_kernel,
        grid_spec=grid_spec,
        out_shape=[
            jax.ShapeDtypeStruct((blocks, 8 * rows, 128), F32),
            jax.ShapeDtypeStruct((blocks, 8 * rows, 128), F32),
            jax.ShapeDtypeStruct((blocks, 128, 128), F32),
            jax.ShapeDtypeStruct((4 * blocks, 40, 128), BF16),
        ],
        compiler_params=pltpu.CompilerParams(dimension_semantics=("arbitrary",)),
        name="scan",
    )(where, mine, other, gain, xc, d_own, d_oth)


def link_kernel(ends_ref, log_ref, start_ref):
    count = ends_ref.shape[0]
    rate = -LOG2E * jnp.exp(log_ref[...])
    rate = jnp.concatenate([rate[:, 0:128], rate[:, 128:256]], 0)
    state = jnp.zeros((32, 128), F32)
    for s in range(count):
        start_ref[s] = state.astype(BF16)
        sums = ends_ref[s, 32:40, :].astype(F32)
        sums = sums[0:2] + sums[2:4]
        spread = jnp.concatenate([jnp.broadcast_to(sums[0:1], (16, 128)), jnp.broadcast_to(sums[1:2], (16, 128))], 0)
        state = jnp.exp2(rate * spread) * state + ends_ref[s, 0:32, :].astype(F32)


def link(ends, a_log):
    return pl.pallas_call(
        link_kernel,
        out_shape=jax.ShapeDtypeStruct((ends.shape[0], 32, 128), BF16),
        name="link",
    )(ends, a_log)


def close_kernel(step_ref, y_ref, rate_ref, start_ref, mine_ref, other_ref, gate_ref, out_ref, s_scr, y_scr, c_ref):
    rows = gate_ref.shape[0]

    @pl.when(pl.program_id(0) == 0)
    def _():
        spread(mine_ref[...] + other_ref[...], 272, 16, c_ref)

    for j in range(8):
        s_scr[16 * j : 16 * j + 16, :] = start_ref[j // 2, (j % 2) * 16 : (j % 2) * 16 + 16, :].astype(F32)
    starts = [s_scr[pl.ds(n, 8, stride=16), :] for n in range(16)]
    rates = [rate_ref[0, 8 * n : 8 * n + 8, :] for n in range(16)]

    def advance(t, total):
        at = pl.multiple_of(t * 8, 8)
        total = total + step_ref[0, pl.ds(at, 8), :]
        even = y_ref[0, pl.ds(at, 8), :]
        odd = None
        for n in range(16):
            c = row_of(c_ref, n * rows + t)
            part = c * starts[n] * jnp.exp2(total * rates[n])
            if n % 2:
                odd = part if odd is None else odd + part
            else:
                even = even + part
        y_scr[pl.ds(at, 8), :] = even + odd
        return total

    lax.fori_loop(0, rows, advance, jnp.zeros((8, 128), F32), unroll=8)
    for j in range(8):
        for i in range(rows // 16):
            low = y_scr[pl.ds(128 * i + j, 8, stride=8), :]
            up = y_scr[pl.ds(128 * i + 64 + j, 8, stride=8), :]
            y = jnp.concatenate([low, up], 0).astype(BF16).astype(F32)
            gate = gate_ref[16 * i : 16 * i + 16, j * 128 : (j + 1) * 128].astype(F32)
            out_ref[16 * i : 16 * i + 16, j * 128 : (j + 1) * 128] = (y * silu(gate)).astype(BF16)


def close(step, y, rate, start, mine, other, gate):
    rows, inner = gate.shape
    return pl.pallas_call(
        close_kernel,
        grid=(inner // BLK,),
        in_specs=[
            pl.BlockSpec((1, 8 * rows, 128), lambda b: (b, 0, 0)),
            pl.BlockSpec((1, 8 * rows, 128), lambda b: (b, 0, 0)),
            pl.BlockSpec((1, 128, 128), lambda b: (b, 0, 0)),
            pl.BlockSpec((4, 32, 128), lambda b: (b, 0, 0)),
            pl.BlockSpec((rows, 288), lambda b: (0, 0)),
            pl.BlockSpec((rows, 288), lambda b: (0, 0)),
            pl.BlockSpec((rows, BLK), lambda b: (0, b)),
        ],
        out_specs=pl.BlockSpec((rows, BLK), lambda b: (0, b)),
        out_shape=jax.ShapeDtypeStruct((rows, inner), BF16),
        scratch_shapes=[pltpu.VMEM((128, 128), F32), pltpu.VMEM((8 * rows, 128), F32), pltpu.VMEM((16 * rows, 128), F32)],
        compiler_params=pltpu.CompilerParams(dimension_semantics=("arbitrary",)),
        name="close",
    )(step, y, rate, start, mine, other, gate)


def from_everyone(x, axis):
    copies = jnp.broadcast_to(x, (lax.axis_size(axis), *x.shape))
    return lax.all_to_all(copies, axis, split_axis=0, concat_axis=0, tiled=True)


def pack_x(core, x_weight):
    return lax.dynamic_slice_in_dim(x_weight.T, core * 128, 128, 1)


def pack_d(core, quarter, dt_weight, dt_bias, a_log, skip, conv_weight, conv_bias):
    part = lax.dynamic_slice_in_dim(dt_weight, core * 128 + quarter * 32, 32, 0)
    logs = lax.dynamic_slice_in_dim(a_log, core * 8 + quarter * 2, 2, 0)
    vec = jnp.where(core == 0, dt_bias, skip)[None, :]
    pieces = [part, *two_parts(logs), *two_parts(vec), jnp.zeros((2, SHARD), BF16)]
    pieces += [conv_weight, conv_bias[None, :], jnp.zeros((3, SHARD), BF16)]
    return jnp.concatenate(pieces, 0)


def shifted(block, axis, by):
    count = lax.axis_size(axis)
    return lax.ppermute(block, axis, [(i, (i + by) % count) for i in range(count)])


def placed(blocks, at, axis):
    count = lax.axis_size(axis)
    here = lax.axis_index(axis)
    first = blocks[0]
    out = jnp.zeros((count, *first.shape), first.dtype)
    for block, (by, row) in zip(blocks, at):
        out = lax.dynamic_update_slice(out, block[None], ((here + by) % count, row) + (0,) * (first.ndim - 1))
    return out


def from_opposite(core, up, down, axis):
    count = lax.axis_size(axis)
    pairs = [(2 * i + c, 2 * ((i + 1 - 2 * c) % count) + c) for i in range(count) for c in range(2)]
    return lax.ppermute(jnp.where(core == 0, up, down), (axis, "core"), pairs)


def both_ways(pair, axis):
    return shifted(pair[0], axis, 1), shifted(pair[1], axis, -1)


def body(conv_input, gate_input, conv_weight, conv_bias, x_weight, dt_gain, dt_weight, dt_bias, a_log, skip):
    core = lax.axis_index("core")
    count = lax.axis_size(SEQ)
    swap = [(0, 1), (1, 0)]
    where = jnp.stack([core, lax.axis_index("z")]).astype(jnp.int32)
    x_piece = pack_x(core, x_weight)
    x_pieces = [x_piece] + [shifted(x_piece, "y", k) for k in (1, 2, 3)]
    x0 = placed(x_pieces, [(0, 0), (-1, 0), (-2, 0), (-3, 0)], "y")
    quarter = lax.axis_index("x")
    d_part = from_everyone(pack_d(core, quarter, dt_weight, dt_bias, a_log, skip, conv_weight, conv_bias), "z")
    d_part = d_part.reshape(8, 48, SHARD)
    prior = lax.ppermute(conv_input[conv_input.shape[0] - 8 :], SEQ, [(i, i + 1) for i in range(count - 1)])
    x1 = both_ways((x0, x0), "z")
    taps = from_everyone(d_part[:, 40:], "y").reshape(4, 8, 8, SHARD)
    x2 = both_ways(x1, "z")
    d0 = from_everyone(d_part[:, :40], "x").reshape(4, 8, 40, SHARD)
    up, down = both_ways((d0, d0), "y")
    xc, lend = conv(where, conv_input, prior, taps)
    x3 = both_ways(x2, "z")
    lent = lax.ppermute(lend, "core", swap)
    x4 = from_opposite(core, *x3, "z")
    d2 = from_opposite(core, up, down, "y")
    d_own = placed([d0, up, down, d2], [(0, 0), (-1, 0), (1, 0), (2, 0)], "y")
    d_oth = lax.ppermute(d_own, "core", swap)
    mine, other = project(where, xc, lent, [x0, *x1, *x2, *x3, x4])
    other = lax.ppermute(other, "core", swap)
    step, y, rate, ends = scan(where, mine, other, dt_gain[None, :], xc, d_own, d_oth)
    ends = lax.all_to_all(ends, SEQ, split_axis=0, concat_axis=0, tiled=True)
    start = lax.all_to_all(link(ends, a_log), SEQ, split_axis=0, concat_axis=0, tiled=True)
    return close(step, y, rate, start, mine, other, gate_input)


def solution(mesh):
    inner = Mesh(mesh.devices.reshape(4, 8, 4, 2), ("y", "z", "x", "core"))
    tokens = P(("x", "core", "y", "z"), None)
    return jax.shard_map(
        body,
        mesh=inner,
        in_specs=(tokens, tokens, P(None, SEQ), P(SEQ), P(SEQ, None), P(), P(None, SEQ), P(SEQ), P(None, SEQ), P(SEQ)),
        out_specs=tokens,
        check_vma=False,
    )
```
